8 devices in a mesh: rep: 1 (over z), dp: 8 (over x, y, core).
Axes of the slice: x: 2, y: 2, z: 1, core: 2. Of those that a mesh axis runs over, the one named last changes fastest.
Arguments:
- g_w_gate: bfloat16 [8, 2, 1280, 5120], P(('rep', 'dp'))
- g_w_up: bfloat16 [8, 2, 1280, 5120], P(('rep', 'dp'))
- g_w_down: bfloat16 [8, 2, 5120, 1280], P(('rep', 'dp'))
- w_gate: bfloat16 [2, 1280, 5120], replicated
- w_up: bfloat16 [2, 1280, 5120], replicated
- w_down: bfloat16 [2, 5120, 1280], replicated
- m_w_gate: float32 [2, 1280, 5120], P(None, 'dp')
- m_w_up: float32 [2, 1280, 5120], P(None, 'dp')
- m_w_down: float32 [2, 5120, 1280], P(None, 'dp')
- v_w_gate: float32 [2, 1280, 5120], P(None, 'dp')
- v_w_up: float32 [2, 1280, 5120], P(None, 'dp')
- v_w_down: float32 [2, 5120, 1280], P(None, 'dp')
Outputs:
- output 1: bfloat16 [2, 1280, 5120], P('rep')
- output 2: bfloat16 [2, 1280, 5120], P('rep')
- output 3: bfloat16 [2, 5120, 1280], P('rep')
- output 4: float32 [2, 1280, 5120], P('rep', 'dp')
- output 5: float32 [2, 1280, 5120], P('rep', 'dp')
- output 6: float32 [2, 5120, 1280], P('rep', 'dp')
- output 7: float32 [2, 1280, 5120], P('rep', 'dp')
- output 8: float32 [2, 1280, 5120], P('rep', 'dp')
- output 9: float32 [2, 5120, 1280], P('rep', 'dp')
All inputs are finite; a program needn't handle non-finite values.
Results may differ from the reference program's by a relative error of at most 0.022.
Values are sent between devices in bfloat16 or wider.
A program may use at most 2 GiB of HBM per device.

```python
import jax
import jax.numpy as jnp
from jax import lax

DEVICES = 8
D = 1280
FF = 5120
LAYERS = 2
NAMES = ("w_gate", "w_up", "w_down")
SHAPES = {"w_gate": (LAYERS, D, FF), "w_up": (LAYERS, D, FF), "w_down": (LAYERS, FF, D)}


def setup_inputs(seed: int = 0, part: int = 0) -> dict:
    kz, *keys = jax.random.split(jax.random.key(seed), 1 + 5 * len(NAMES))
    loud = 2.0 ** jax.random.uniform(kz, (), jnp.float32, -1.0, 1.0)
    drawn = {}
    for name, key, both in zip(NAMES, keys[:3], keys[3:6], strict=True):
        own = jax.random.normal(jax.random.fold_in(key, part), (DEVICES, *SHAPES[name]), jnp.float32)
        shared = jax.random.normal(jax.random.fold_in(both, part), SHAPES[name], jnp.float32)
        drawn["g_" + name] = (loud * (0.7 * shared / DEVICES + 0.7 * own * DEVICES**-0.5)).astype(jnp.bfloat16)
    for name, key in zip(NAMES, keys[6:9], strict=True):
        drawn[name] = (jax.random.normal(key, SHAPES[name], jnp.float32) * SHAPES[name][1] ** -0.5).astype(jnp.bfloat16)
    for name, key in zip(NAMES, keys[9:12], strict=True):
        drawn["m_" + name] = loud * 0.5 * jax.random.normal(key, SHAPES[name], jnp.float32)
    for name, key in zip(NAMES, keys[12:15], strict=True):
        drawn["v_" + name] = loud * loud * jax.random.uniform(key, SHAPES[name], jnp.float32, 0.5, 1.5)
    return drawn


def adamw(w, m, v, g):
    m = 0.9 * m + 0.1 * g
    v = 0.95 * v + 0.05 * g * g
    step = m * lax.rsqrt(v + 1e-8) + 0.1 * w
    return (w - 0.02 * step).astype(jnp.bfloat16), m, v


def clipped(gradients, sum_of_squares, count):
    factor = jnp.minimum(1.0, 0.5 * lax.rsqrt(sum_of_squares / count + 1e-30))
    return [g * factor for g in gradients]


def reference(g_w_gate, g_w_up, g_w_down, w_gate, w_up, w_down, m_w_gate, m_w_up, m_w_down, v_w_gate, v_w_up, v_w_down):
    def total(terms):
        return lax.scan(lambda so_far, term: (so_far + term.astype(jnp.float32), None), jnp.zeros(terms.shape[1:], jnp.float32), terms)[0]

    gradients = [total(terms).astype(jnp.bfloat16).astype(jnp.float32) for terms in (g_w_gate, g_w_up, g_w_down)]
    gradients = clipped(gradients, sum(jnp.sum(g * g) for g in gradients), sum(g.size for g in gradients))
    new = [
        adamw(w.astype(jnp.float32), m, v, g)
        for w, m, v, g in zip((w_gate, w_up, w_down), (m_w_gate, m_w_up, m_w_down), (v_w_gate, v_w_up, v_w_down), gradients, strict=True)
    ]
    return tuple(one[which] for which in range(3) for one in new)
```

```python
import functools

import jax
import jax.numpy as jnp
from jax import lax
from jax.experimental import pallas as pl
from jax.experimental.pallas import tpu as pltpu
from jax.sharding import PartitionSpec as P

MESH = pl.DeviceIdType.MESH
F32, BF16 = jnp.float32, jnp.bfloat16
CHIPS = ((1, 1), (1, 0), (0, 1), (0, 0))


def adamw(w, m, v, g):
    m = 0.9 * m + 0.1 * g
    v = 0.95 * v + 0.05 * g * g
    step = m * lax.rsqrt(v + 1e-8) + 0.1 * w
    return (w - 0.02 * step).astype(BF16), m, v


def place(dx=0, dy=0, dc=0):
    me = lax.axis_index("dp")
    x, y, c = me // 4, lax.rem(me // 2, 2), lax.rem(me, 2)
    x = 1 - x if dx else x
    y = 1 - y if dy else y
    c = 1 - c if dc else c
    return 4 * x + 2 * y + c


def rows_of(ref, half, total):
    return ref.at[pl.ds(half * total, total)]


def add_into(dst, parts, lanes):
    def body(i, carry):
        s = pl.ds(pl.multiple_of(i * 16, 16), 16)
        total = parts[0][s, :].astype(F32)
        for p in parts[1:]:
            total = total + p[s, :].astype(F32)
        dst[s, :] = total.astype(BF16)
        return carry

    lax.fori_loop(0, dst.shape[0] // 16, body, 0)


def add_square(dst, parts, lanes, acc):
    def body(i, carry):
        s = pl.ds(pl.multiple_of(i * 16, 16), 16)
        total = parts[0][s, :].astype(F32)
        for p in parts[1:]:
            total = total + p[s, :].astype(F32)
        total = total.astype(BF16)
        dst[s, :] = total
        total = total.astype(F32)
        for k in range(lanes // 128):
            one = total[:, k * 128 : (k + 1) * 128]
            carry = carry + one * one
        return carry

    acc[...] += lax.fori_loop(0, dst.shape[0] // 16, body, jnp.zeros((16, 128), F32))


def sum_kernel(shapes, *refs):
    g, refs = refs[:3], refs[3:]
    out, squares, refs = refs[:3], refs[3], refs[4:]
    near, refs = refs[:3], refs[3:]
    snd, rcv, own, par, refs = refs[0:2], refs[2:4], refs[4:6], refs[6:8], refs[8:]
    acc, norms, d2d_s, d2d_r, link_s, link_r, own_sem, par_sem, out_sem, norm_s, norm_r = refs
    layers = g[0].shape[1]
    units = [(a, l) for a in range(3) for l in range(layers)]
    kind = [0, 0, 1]
    slot = {}
    for a, l in units:
        slot[a, l] = sum(1 for u in slot if kind[u[0]] == kind[a])
    me = lax.axis_index("dp")
    rep = lax.axis_index("rep")
    xn, yn, cn = place(dx=1), place(dy=1), place(dc=1)

    barrier = pltpu.get_barrier_semaphore()
    others = [lax.rem(me + k, 8) for k in range(1, 8)]
    for d in others:
        pl.semaphore_signal(barrier, inc=1, device_id=(rep, d), device_id_type=MESH)
    pl.semaphore_wait(barrier, 7)

    def half_of(u, device, h):
        a, l = u
        n = shapes[a][0] // 2
        return g[a].at[0, l, pl.ds(pl.multiple_of(device * (2 * n) + h * n, 16), n)]

    d2d = {}
    for i, u in enumerate(units):
        for s, (dx, dy) in enumerate(CHIPS):
            for h in range(2):
                d2d[i, s, h] = pltpu.make_async_remote_copy(
                    src_ref=half_of(u, place(dx, dy, 1), h),
                    dst_ref=near[u[0]].at[u[1], s, h],
                    send_sem=d2d_s.at[i, s, h],
                    recv_sem=d2d_r.at[i, s, h],
                    device_id=(rep, cn),
                    device_id_type=MESH,
                )
                d2d[i, s, h].start()

    tasks = []
    for i in range(len(units)):
        tasks += [(i, 0, 0, (), 0), (i, 0, 1, (), 1), (i, 1, 0, (), 2), (i, 2, 1, (), 3)]
    for i in range(len(units)):
        tasks += [(i, 1, 1, (1,), 4), (i, 2, 0, (0,), 5)]
    for i in range(len(units)):
        tasks += [(i, 3, 0, (2, 5), None), (i, 3, 1, (3, 4), None)]

    link = {}

    def link_copy(i, j):
        a, l = units[i]
        k = kind[a]
        return pltpu.make_async_remote_copy(
            src_ref=snd[k].at[slot[a, l], j % 4],
            dst_ref=rcv[k].at[slot[a, l], j],
            send_sem=link_s.at[i, j],
            recv_sem=link_r.at[i, j],
            device_id=(rep, xn if j % 2 == 0 else yn),
            device_id_type=MESH,
        )

    loads = {}

    def load(t):
        i, s, h, _, _ = tasks[t]
        a, l = units[i]
        k = kind[a]
        b = t % 2
        mine = pltpu.make_async_copy(half_of(units[i], place(*CHIPS[s], 0), h), own[k].at[b], own_sem.at[b])
        mine.start()
        d2d[i, s, h].wait_recv()
        theirs = pltpu.make_async_copy(near[a].at[l, s, h], par[k].at[b], par_sem.at[b])
        theirs.start()
        loads[t] = (mine, theirs)

    acc[...] = jnp.zeros_like(acc)
    load(0)
    stores = []
    for t, (i, s, h, arrived, j) in enumerate(tasks):
        if t + 1 < len(tasks):
            load(t + 1)
        a, l = units[i]
        k = kind[a]
        lanes = shapes[a][1]
        for one in loads[t]:
            one.wait()
        for r in arrived:
            link_copy(i, r).wait_recv()
        parts = [own[k].at[t % 2], par[k].at[t % 2]] + [rcv[k].at[slot[a, l], r] for r in arrived]
        if j is None:
            dst = snd[k].at[slot[a, l], 2 + h]
            link[i, 2 + h].wait_send()
            add_square(dst, parts, lanes, acc)
            n = shapes[a][0] // 2
            store = pltpu.make_async_copy(dst, out[a].at[l, pl.ds(h * n, n)], out_sem.at[i, h])
            store.start()
            stores.append(store)
        else:
            dst = snd[k].at[slot[a, l], j % 4]
            if j >= 4:
                link[i, j - 4].wait_send()
            add_into(dst, parts, lanes)
            link[i, j] = link_copy(i, j)
            link[i, j].start()

    sent = []
    for k in range(1, 8):
        to = lax.rem(me + k, 8)
        copy = pltpu.make_async_remote_copy(
            src_ref=acc, dst_ref=norms.at[me], send_sem=norm_s.at[k - 1], recv_sem=norm_r.at[k - 1], device_id=(rep, to), device_id_type=MESH
        )
        copy.start()
        sent.append(copy)
    norms[me] = acc[...]
    for copy in sent:
        copy.wait_recv()
    total = norms[0]
    for d in range(1, 8):
        total = total + norms[d]
    squares[...] = jnp.full(squares.shape, jnp.sum(total), F32)
    for copy in sent:
        copy.wait_send()
    for store in stores:
        store.wait()
    for copy in d2d.values():
        copy.wait_send()
    for i in range(len(units)):
        for j in (4, 5):
            link[i, j].wait_send()


def summed(terms):
    layers = terms[0].shape[1]
    shapes = [(t.shape[2] // 8, t.shape[3]) for t in terms]
    halves = [(shapes[0][0] // 2, shapes[0][1]), (shapes[2][0] // 2, shapes[2][1])]
    count = [2 * layers, layers]
    any_ = pl.BlockSpec(memory_space=pl.ANY)
    outs = pl.pallas_call(
        functools.partial(sum_kernel, shapes),
        out_shape=[jax.ShapeDtypeStruct((layers, *s), BF16) for s in shapes]
        + [jax.ShapeDtypeStruct((8, 128), F32)]
        + [jax.ShapeDtypeStruct((layers, 4, 2, s[0] // 2, s[1]), BF16) for s in shapes],
        in_specs=[any_] * 3,
        out_specs=[any_] * 3 + [pl.BlockSpec(memory_space=pltpu.VMEM)] + [any_] * 3,
        scratch_shapes=[pltpu.VMEM((n, 4, *s), BF16) for n, s in zip(count, halves)]
        + [pltpu.VMEM((n, 6, *s), BF16) for n, s in zip(count, halves)]
        + [pltpu.VMEM((2, *s), BF16) for s in halves] * 2
        + [
            pltpu.VMEM((16, 128), F32),
            pltpu.VMEM((8, 16, 128), F32),
            pltpu.SemaphoreType.DMA((3 * layers, 4, 2)),
            pltpu.SemaphoreType.DMA((3 * layers, 4, 2)),
            pltpu.SemaphoreType.DMA((3 * layers, 6)),
            pltpu.SemaphoreType.DMA((3 * layers, 6)),
            pltpu.SemaphoreType.DMA((2,)),
            pltpu.SemaphoreType.DMA((2,)),
            pltpu.SemaphoreType.DMA((3 * layers, 2)),
            pltpu.SemaphoreType.DMA((7,)),
            pltpu.SemaphoreType.DMA((7,)),
        ],
        compiler_params=pltpu.CompilerParams(collective_id=0, has_side_effects=True, vmem_limit_bytes=62 * 1024 * 1024),
        name="sum_terms",
    )(*terms)
    return outs[:3], outs[3][0, 0]


def clipped(gradients, sum_of_squares, count):
    factor = jnp.minimum(1.0, 0.5 * lax.rsqrt(sum_of_squares / count + 1e-30))
    return [g * factor for g in gradients]


def solution(mesh):
    def step(*arrays):
        terms, weights, m, v = (arrays[i : i + 3] for i in (0, 3, 6, 9))
        gradients, squares = summed(terms)
        gradients = [g.astype(F32) for g in gradients]
        gradients = clipped(gradients, squares, 8 * sum(g.size for g in gradients))
        me = lax.axis_index("dp")
        own = [lax.dynamic_slice_in_dim(w, me * one.shape[1], one.shape[1], 1).astype(F32) for w, one in zip(weights, m)]
        new = [adamw(w, m, v, g) for w, m, v, g in zip(own, m, v, gradients)]
        whole = [lax.all_gather(one[0], "dp", axis=1, tiled=True) for one in new]
        return (*whole, *(one[1] for one in new), *(one[2] for one in new))

    all_of, cut = P(None, None, None), P(None, "dp", None)
    return jax.shard_map(
        step,
        mesh=mesh,
        in_specs=(P(("rep", "dp"), None, None, None),) * 3 + (all_of,) * 3 + (cut,) * 6,
        out_specs=(P("rep", None, None),) * 3 + (P("rep", "dp", None),) * 6,
        check_vma=False,
    )
```

```python
import functools

import jax
import jax.numpy as jnp
from jax import lax
from jax.experimental import pallas as pl
from jax.experimental.pallas import tpu as pltpu
from jax.sharding import PartitionSpec as P


MESH = pl.DeviceIdType.MESH
F32, BF16 = jnp.float32, jnp.bfloat16
CHIPS = ((1, 1), (1, 0), (0, 1), (0, 0))


def place(dx=0, dy=0, dc=0):
    me = lax.axis_index("dp")
    x, y, c = me // 4, lax.rem(me // 2, 2), lax.rem(me, 2)
    x = 1 - x if dx else x
    y = 1 - y if dy else y
    c = 1 - c if dc else c
    return 4 * x + 2 * y + c


def add_into(dst, parts):
    def body(i, carry):
        s = pl.ds(pl.multiple_of(i * 16, 16), 16)
        total = parts[0][s, :].astype(F32)
        for p in parts[1:]:
            total = total + p[s, :].astype(F32)
        dst[s, :] = total.astype(BF16)
        return carry

    lax.fori_loop(0, dst.shape[0] // 16, body, 0)


def add_square(dst, parts, lanes, acc):
    def body(i, carry):
        s = pl.ds(pl.multiple_of(i * 16, 16), 16)
        total = parts[0][s, :].astype(F32)
        for p in parts[1:]:
            total = total + p[s, :].astype(F32)
        total = total.astype(BF16)
        dst[s, :] = total
        total = total.astype(F32)
        for k in range(lanes // 128):
            one = total[:, k * 128 : (k + 1) * 128]
            carry = carry + one * one
        return carry

    acc[...] += lax.fori_loop(0, dst.shape[0] // 16, body, jnp.zeros((16, 128), F32))


def sum_kernel(shapes, *refs):
    g, refs = refs[:3], refs[3:]
    out, squares, refs = refs[:3], refs[3], refs[4:]
    near, refs = refs[:3], refs[3:]
    snd, rcv, own, par, refs = refs[0:2], refs[2:4], refs[4:6], refs[6:8], refs[8:]
    acc, norms, d2d_s, d2d_r, link_s, link_r, own_sem, par_sem, out_sem, norm_s, norm_r = refs
    layers = g[0].shape[1]
    units = [(a, l) for a in range(3) for l in range(layers)]
    kind = [0, 0, 1]
    slot = {}
    for a, l in units:
        slot[a, l] = sum(1 for u in slot if kind[u[0]] == kind[a])
    me = lax.axis_index("dp")
    rep = lax.axis_index("rep")
    xn, yn, cn = place(dx=1), place(dy=1), place(dc=1)

    barrier = pltpu.get_barrier_semaphore()
    others = [lax.rem(me + k, 8) for k in range(1, 8)]
    for d in others:
        pl.semaphore_signal(barrier, inc=1, device_id=(rep, d), device_id_type=MESH)
    pl.semaphore_wait(barrier, 7)

    def half_of(u, device, h):
        a, l = u
        n = shapes[a][0] // 2
        return g[a].at[0, l, pl.ds(pl.multiple_of(device * (2 * n) + h * n, 16), n)]

    d2d = {}
    for i, u in enumerate(units):
        for s, (dx, dy) in enumerate(CHIPS):
            for h in range(2):
                d2d[i, s, h] = pltpu.make_async_remote_copy(
                    src_ref=half_of(u, place(dx, dy, 1), h),
                    dst_ref=near[u[0]].at[u[1], s, h],
                    send_sem=d2d_s.at[i, s, h],
                    recv_sem=d2d_r.at[i, s, h],
                    device_id=(rep, cn),
                    device_id_type=MESH,
                )
                d2d[i, s, h].start()

    tasks = []
    for i in range(len(units)):
        tasks += [(i, 0, 0, (), 0), (i, 0, 1, (), 1), (i, 1, 0, (), 2), (i, 2, 1, (), 3)]
    for i in range(len(units)):
        tasks += [(i, 1, 1, (1,), 4), (i, 2, 0, (0,), 5)]
    for i in range(len(units)):
        tasks += [(i, 3, 0, (2, 5), None), (i, 3, 1, (3, 4), None)]

    link = {}

    def link_copy(i, j):
        a, l = units[i]
        k = kind[a]
        return pltpu.make_async_remote_copy(
            src_ref=snd[k].at[slot[a, l], j % 4],
            dst_ref=rcv[k].at[slot[a, l], j],
            send_sem=link_s.at[i, j],
            recv_sem=link_r.at[i, j],
            device_id=(rep, xn if j % 2 == 0 else yn),
            device_id_type=MESH,
        )

    loads = {}

    def load(t):
        i, s, h, _, _ = tasks[t]
        a, l = units[i]
        k = kind[a]
        b = t % 2
        mine = pltpu.make_async_copy(half_of(units[i], place(*CHIPS[s], 0), h), own[k].at[b], own_sem.at[b])
        mine.start()
        d2d[i, s, h].wait_recv()
        theirs = pltpu.make_async_copy(near[a].at[l, s, h], par[k].at[b], par_sem.at[b])
        theirs.start()
        loads[t] = (mine, theirs)

    acc[...] = jnp.zeros_like(acc)
    load(0)
    stores = []
    for t, (i, s, h, arrived, j) in enumerate(tasks):
        if t + 1 < len(tasks):
            load(t + 1)
        a, l = units[i]
        k = kind[a]
        lanes = shapes[a][1]
        for one in loads[t]:
            one.wait()
        for r in arrived:
            link_copy(i, r).wait_recv()
        parts = [own[k].at[t % 2], par[k].at[t % 2]] + [rcv[k].at[slot[a, l], r] for r in arrived]
        if j is None:
            dst = snd[k].at[slot[a, l], 2 + h]
            link[i, 2 + h].wait_send()
            add_square(dst, parts, lanes, acc)
            n = shapes[a][0] // 2
            store = pltpu.make_async_copy(dst, out[a].at[l, pl.ds(h * n, n)], out_sem.at[i, h])
            store.start()
            stores.append(store)
        else:
            dst = snd[k].at[slot[a, l], j % 4]
            if j >= 4:
                link[i, j - 4].wait_send()
            add_into(dst, parts)
            link[i, j] = link_copy(i, j)
            link[i, j].start()

    sent = []
    for k in range(1, 8):
        to = lax.rem(me + k, 8)
        copy = pltpu.make_async_remote_copy(
            src_ref=acc, dst_ref=norms.at[me], send_sem=norm_s.at[k - 1], recv_sem=norm_r.at[k - 1], device_id=(rep, to), device_id_type=MESH
        )
        copy.start()
        sent.append(copy)
    norms[me] = acc[...]
    for copy in sent:
        copy.wait_recv()
    total = norms[0]
    for d in range(1, 8):
        total = total + norms[d]
    squares[...] = jnp.full(squares.shape, jnp.sum(total), F32)
    for copy in sent:
        copy.wait_send()
    for store in stores:
        store.wait()
    for copy in d2d.values():
        copy.wait_send()
    for i in range(len(units)):
        for j in (4, 5):
            link[i, j].wait_send()


def summed(terms):
    layers = terms[0].shape[1]
    shapes = [(t.shape[2] // 8, t.shape[3]) for t in terms]
    halves = [(shapes[0][0] // 2, shapes[0][1]), (shapes[2][0] // 2, shapes[2][1])]
    count = [2 * layers, layers]
    any_ = pl.BlockSpec(memory_space=pl.ANY)
    outs = pl.pallas_call(
        functools.partial(sum_kernel, shapes),
        out_shape=[jax.ShapeDtypeStruct((layers, *s), BF16) for s in shapes]
        + [jax.ShapeDtypeStruct((8, 128), F32)]
        + [jax.ShapeDtypeStruct((layers, 4, 2, s[0] // 2, s[1]), BF16) for s in shapes],
        in_specs=[any_] * 3,
        out_specs=[any_] * 3 + [pl.BlockSpec(memory_space=pltpu.VMEM)] + [any_] * 3,
        scratch_shapes=[pltpu.VMEM((n, 4, *s), BF16) for n, s in zip(count, halves)]
        + [pltpu.VMEM((n, 6, *s), BF16) for n, s in zip(count, halves)]
        + [pltpu.VMEM((2, *s), BF16) for s in halves] * 2
        + [
            pltpu.VMEM((16, 128), F32),
            pltpu.VMEM((8, 16, 128), F32),
            pltpu.SemaphoreType.DMA((3 * layers, 4, 2)),
            pltpu.SemaphoreType.DMA((3 * layers, 4, 2)),
            pltpu.SemaphoreType.DMA((3 * layers, 6)),
            pltpu.SemaphoreType.DMA((3 * layers, 6)),
            pltpu.SemaphoreType.DMA((2,)),
            pltpu.SemaphoreType.DMA((2,)),
            pltpu.SemaphoreType.DMA((3 * layers, 2)),
            pltpu.SemaphoreType.DMA((7,)),
            pltpu.SemaphoreType.DMA((7,)),
        ],
        compiler_params=pltpu.CompilerParams(collective_id=0, has_side_effects=True, vmem_limit_bytes=62 * 1024 * 1024),
        name="sum_terms",
    )(*terms)
    return outs[:3], outs[3]


def step_kernel(count, me, squares, g, w, m, v, *rest):
    new_w, new_m, new_v = rest[-3:]
    factor = jnp.minimum(1.0, 0.5 * lax.rsqrt(squares[:1, :1] / count + 1e-30))
    g = g[0].astype(F32) * factor
    m = 0.9 * m[0] + 0.1 * g
    v = 0.95 * v[0] + 0.05 * g * g
    w = w[0].astype(F32)
    step = m * lax.rsqrt(v + 1e-8) + 0.1 * w
    new_w[...] = (w - 0.02 * step).astype(BF16)
    new_m[0] = m
    new_v[0] = v


def stepped(me, squares, count, layer, g, w, m, v, before):
    rows, lanes = g.shape[1:]
    n = rows // 5
    here = pl.BlockSpec((1, n, lanes), lambda i, me: (layer, i, 0))
    specs = [
        pl.BlockSpec((8, 128), lambda i, me: (0, 0)),
        here,
        pl.BlockSpec((1, n, lanes), lambda i, me: (layer, me[0] * 5 + i, 0)),
        here,
        here,
    ]
    moment = jax.ShapeDtypeStruct(m.shape, F32)
    return pl.pallas_call(
        functools.partial(step_kernel, count),
        out_shape=[jax.ShapeDtypeStruct((rows, lanes), BF16), moment, moment],
        grid_spec=pltpu.PrefetchScalarGridSpec(
            num_scalar_prefetch=1,
            grid=(5,),
            in_specs=specs + [pl.BlockSpec(memory_space=pl.ANY)] * len(before),
            out_specs=[pl.BlockSpec((n, lanes), lambda i, me: (i, 0)), here, here],
        ),
        input_output_aliases={6 + i: 1 + i for i in range(len(before))},
        cost_estimate=pl.CostEstimate(flops=15 * rows * lanes, bytes_accessed=22 * rows * lanes, transcendentals=rows * lanes),
        name="adamw",
    )(me, squares, g, w, m, v, *before)


def place_kernel(layer, offsets, n_before, *refs):
    n = len(offsets)
    blocks, out = refs[:n], refs[n + n_before]
    held, in_sem, out_sem = refs[n + n_before + 1 :]
    rows = blocks[0].shape[0]
    loads = [pltpu.make_async_copy(b, held.at[i], in_sem.at[i]) for i, b in enumerate(blocks)]
    for one in loads:
        one.start()
    stores = []
    for i, offset in enumerate(offsets):
        loads[i].wait()
        at = pl.multiple_of(place(*offset) * rows, 16)
        stores.append(pltpu.make_async_copy(held.at[i], out.at[layer, pl.ds(at, rows)], out_sem.at[i]))
        stores[-1].start()
    for one in stores:
        one.wait()


def placed(blocks, offsets, layer, shape, before):
    n = len(blocks)
    any_ = pl.BlockSpec(memory_space=pl.ANY)
    return pl.pallas_call(
        functools.partial(place_kernel, layer, offsets, len(before)),
        out_shape=jax.ShapeDtypeStruct(shape, BF16),
        in_specs=[any_] * (n + len(before)),
        out_specs=any_,
        scratch_shapes=[pltpu.VMEM((n, *blocks[0].shape), BF16), pltpu.SemaphoreType.DMA((n,)), pltpu.SemaphoreType.DMA((n,))],
        input_output_aliases={n: 0} if before else {},
        cost_estimate=pl.CostEstimate(flops=0, bytes_accessed=4 * n * blocks[0].size, transcendentals=0),
        name="place",
    )(*blocks, *before)


def send(block, dx=0, dy=0, dc=0):
    flip = 4 * dx + 2 * dy + dc
    return lax.ppermute(block, "dp", [(d, d ^ flip) for d in range(8)])


def solution(mesh):
    def step(*arrays):
        terms, weights, m, v = (arrays[i : i + 3] for i in (0, 3, 6, 9))
        gradients, squares = summed(terms)
        count = 8 * sum(g.size for g in gradients)
        me = lax.axis_index("dp")[None]
        layers = weights[0].shape[0]
        new_m, new_v, whole = [()] * 3, [()] * 3, [()] * 3
        units = [(a, l) for a in range(3) for l in range(layers)]
        first, second = [], []
        for a, l in units:
            before = (new_m[a], new_v[a]) if l else ()
            own, new_m[a], new_v[a] = stepped(me, squares, count, l, gradients[a], weights[a], m[a], v[a], before)
            first.append((own, send(own, dx=1), send(own, dy=1), send(own, dc=1)))
        for i, (own, x, y, c) in enumerate(first):
            far = send(y, dx=1) if i % 2 else send(x, dy=1)
            second.append((far, send(x, dc=1), send(y, dc=1)))
        for i, (a, l) in enumerate(units):
            own, x, y, c = first[i]
            far, xc, yc = second[i]
            places = ((0, 0, 0), (1, 0, 0), (0, 1, 0), (0, 0, 1), (1, 0, 1), (0, 1, 1))
            whole[a] = placed([own, x, y, c, xc, yc], places, l, weights[a].shape, (whole[a],) if l else ())
        for i, (a, l) in enumerate(units):
            far = second[i][0]
            both = [far, send(far, dc=1)]
            whole[a] = placed(both, ((1, 1, 0), (1, 1, 1)), l, weights[a].shape, (whole[a],))
        return (*whole, *new_m, *new_v)

    all_of, cut = P(None, None, None), P(None, "dp", None)
    return jax.shard_map(
        step,
        mesh=mesh,
        in_specs=(P(("rep", "dp"), None, None, None),) * 3 + (all_of,) * 3 + (cut,) * 6,
        out_specs=(P("rep", None, None),) * 3 + (P("rep", "dp", None),) * 6,
        check_vma=False,
    )
```

```python
import functools

import jax
import jax.numpy as jnp
from jax import lax
from jax.experimental import pallas as pl
from jax.experimental.pallas import tpu as pltpu
from jax.sharding import PartitionSpec as P


MESH = pl.DeviceIdType.MESH
F32, BF16 = jnp.float32, jnp.bfloat16
CHIPS = ((1, 1), (1, 0), (0, 1), (0, 0))


def place(dx=0, dy=0, dc=0):
    me = lax.axis_index("dp")
    x, y, c = me // 4, lax.rem(me // 2, 2), lax.rem(me, 2)
    x = 1 - x if dx else x
    y = 1 - y if dy else y
    c = 1 - c if dc else c
    return 4 * x + 2 * y + c


def add_into(dst, parts):
    def body(i, carry):
        s = pl.ds(pl.multiple_of(i * 16, 16), 16)
        total = parts[0][s, :].astype(F32)
        for p in parts[1:]:
            total = total + p[s, :].astype(F32)
        dst[s, :] = total.astype(BF16)
        return carry

    lax.fori_loop(0, dst.shape[0] // 16, body, 0)


def add_square(dst, parts, lanes, acc):
    def body(i, carry):
        s = pl.ds(pl.multiple_of(i * 16, 16), 16)
        total = parts[0][s, :].astype(F32)
        for p in parts[1:]:
            total = total + p[s, :].astype(F32)
        total = total.astype(BF16)
        dst[s, :] = total
        total = total.astype(F32)
        for k in range(lanes // 128):
            one = total[:, k * 128 : (k + 1) * 128]
            carry = carry + one * one
        return carry

    acc[...] += lax.fori_loop(0, dst.shape[0] // 16, body, jnp.zeros((16, 128), F32))


def sum_kernel(shapes, *refs):
    g, refs = refs[:3], refs[3:]
    out, squares, refs = refs[:3], refs[3], refs[4:]
    near, refs = refs[:3], refs[3:]
    snd, rcv, own, par, refs = refs[0:2], refs[2:4], refs[4:6], refs[6:8], refs[8:]
    acc, norms, d2d_s, d2d_r, link_s, link_r, own_sem, par_sem, out_sem, norm_s, norm_r = refs
    layers = g[0].shape[1]
    units = [(a, l) for a in range(3) for l in range(layers)]
    kind = [0, 0, 1]
    slot = {}
    for a, l in units:
        slot[a, l] = sum(1 for u in slot if kind[u[0]] == kind[a])
    me = lax.axis_index("dp")
    rep = lax.axis_index("rep")
    xn, yn, cn = place(dx=1), place(dy=1), place(dc=1)

    barrier = pltpu.get_barrier_semaphore()
    others = [lax.rem(me + k, 8) for k in range(1, 8)]
    for d in others:
        pl.semaphore_signal(barrier, inc=1, device_id=(rep, d), device_id_type=MESH)
    pl.semaphore_wait(barrier, 7)

    def half_of(u, device, h):
        a, l = u
        n = shapes[a][0] // 2
        return g[a].at[0, l, pl.ds(pl.multiple_of(device * (2 * n) + h * n, 16), n)]

    d2d = {}
    for i, u in enumerate(units):
        for s, (dx, dy) in enumerate(CHIPS):
            for h in range(2):
                d2d[i, s, h] = pltpu.make_async_remote_copy(
                    src_ref=half_of(u, place(dx, dy, 1), h),
                    dst_ref=near[u[0]].at[u[1], s, h],
                    send_sem=d2d_s.at[i, s, h],
                    recv_sem=d2d_r.at[i, s, h],
                    device_id=(rep, cn),
                    device_id_type=MESH,
                )
                d2d[i, s, h].start()

    tasks = []
    for i in range(len(units)):
        tasks += [(i, 0, 0, (), 0), (i, 0, 1, (), 1), (i, 1, 0, (), 2), (i, 2, 1, (), 3)]
    for i in range(len(units)):
        tasks += [(i, 1, 1, (1,), 4), (i, 2, 0, (0,), 5)]
    for i in range(len(units)):
        tasks += [(i, 3, 0, (2, 5), None), (i, 3, 1, (3, 4), None)]

    link = {}

    def link_copy(i, j):
        a, l = units[i]
        k = kind[a]
        return pltpu.make_async_remote_copy(
            src_ref=snd[k].at[slot[a, l], j % 4],
            dst_ref=rcv[k].at[slot[a, l], j],
            send_sem=link_s.at[i, j],
            recv_sem=link_r.at[i, j],
            device_id=(rep, xn if j % 2 == 0 else yn),
            device_id_type=MESH,
        )

    loads = {}

    def load(t):
        i, s, h, _, _ = tasks[t]
        a, l = units[i]
        k = kind[a]
        b = t % 2
        mine = pltpu.make_async_copy(half_of(units[i], place(*CHIPS[s], 0), h), own[k].at[b], own_sem.at[b])
        mine.start()
        d2d[i, s, h].wait_recv()
        theirs = pltpu.make_async_copy(near[a].at[l, s, h], par[k].at[b], par_sem.at[b])
        theirs.start()
        loads[t] = (mine, theirs)

    acc[...] = jnp.zeros_like(acc)
    load(0)
    stores = []
    for t, (i, s, h, arrived, j) in enumerate(tasks):
        if t + 1 < len(tasks):
            load(t + 1)
        a, l = units[i]
        k = kind[a]
        lanes = shapes[a][1]
        for one in loads[t]:
            one.wait()
        for r in arrived:
            link_copy(i, r).wait_recv()
        parts = [own[k].at[t % 2], par[k].at[t % 2]] + [rcv[k].at[slot[a, l], r] for r in arrived]
        if j is None:
            dst = snd[k].at[slot[a, l], 2 + h]
            link[i, 2 + h].wait_send()
            add_square(dst, parts, lanes, acc)
            n = shapes[a][0] // 2
            store = pltpu.make_async_copy(dst, out[a].at[l, pl.ds(h * n, n)], out_sem.at[i, h])
            store.start()
            stores.append(store)
        else:
            dst = snd[k].at[slot[a, l], j % 4]
            if j >= 4:
                link[i, j - 4].wait_send()
            add_into(dst, parts)
            link[i, j] = link_copy(i, j)
            link[i, j].start()

    sent = []
    for k in range(1, 8):
        to = lax.rem(me + k, 8)
        copy = pltpu.make_async_remote_copy(
            src_ref=acc, dst_ref=norms.at[me], send_sem=norm_s.at[k - 1], recv_sem=norm_r.at[k - 1], device_id=(rep, to), device_id_type=MESH
        )
        copy.start()
        sent.append(copy)
    norms[me] = acc[...]
    for copy in sent:
        copy.wait_recv()
    total = norms[0]
    for d in range(1, 8):
        total = total + norms[d]
    squares[...] = jnp.full(squares.shape, jnp.sum(total), F32)
    for copy in sent:
        copy.wait_send()
    for store in stores:
        store.wait()
    for copy in d2d.values():
        copy.wait_send()
    for i in range(len(units)):
        for j in (4, 5):
            link[i, j].wait_send()


def summed(terms):
    layers = terms[0].shape[1]
    shapes = [(t.shape[2] // 8, t.shape[3]) for t in terms]
    halves = [(shapes[0][0] // 2, shapes[0][1]), (shapes[2][0] // 2, shapes[2][1])]
    count = [2 * layers, layers]
    any_ = pl.BlockSpec(memory_space=pl.ANY)
    outs = pl.pallas_call(
        functools.partial(sum_kernel, shapes),
        out_shape=[jax.ShapeDtypeStruct((layers, *s), BF16) for s in shapes]
        + [jax.ShapeDtypeStruct((8, 128), F32)]
        + [jax.ShapeDtypeStruct((layers, 4, 2, s[0] // 2, s[1]), BF16) for s in shapes],
        in_specs=[any_] * 3,
        out_specs=[any_] * 3 + [pl.BlockSpec(memory_space=pltpu.VMEM)] + [any_] * 3,
        scratch_shapes=[pltpu.VMEM((n, 4, *s), BF16) for n, s in zip(count, halves)]
        + [pltpu.VMEM((n, 6, *s), BF16) for n, s in zip(count, halves)]
        + [pltpu.VMEM((2, *s), BF16) for s in halves] * 2
        + [
            pltpu.VMEM((16, 128), F32),
            pltpu.VMEM((8, 16, 128), F32),
            pltpu.SemaphoreType.DMA((3 * layers, 4, 2)),
            pltpu.SemaphoreType.DMA((3 * layers, 4, 2)),
            pltpu.SemaphoreType.DMA((3 * layers, 6)),
            pltpu.SemaphoreType.DMA((3 * layers, 6)),
            pltpu.SemaphoreType.DMA((2,)),
            pltpu.SemaphoreType.DMA((2,)),
            pltpu.SemaphoreType.DMA((3 * layers, 2)),
            pltpu.SemaphoreType.DMA((7,)),
            pltpu.SemaphoreType.DMA((7,)),
        ],
        compiler_params=pltpu.CompilerParams(collective_id=0, has_side_effects=True, vmem_limit_bytes=62 * 1024 * 1024),
        name="sum_terms",
    )(*terms)
    return outs[:3], outs[3]


def step_kernel(count, with_weight, me, squares, g, w, m, v, *rest):
    new_w, new_m, new_v = rest[-3:]
    w, m, v = stepped_block(squares[:1, :1], count, g[0], w[0], m[0], v[0])
    if with_weight:
        new_w[...] = w
    new_m[0] = m
    new_v[0] = v


def stepped_block(squares, count, g, w, m, v):
    g = g.astype(F32) * jnp.minimum(1.0, 0.5 * lax.rsqrt(squares / count + 1e-30))
    m = 0.9 * m + 0.1 * g
    v = 0.95 * v + 0.05 * g * g
    w = w.astype(F32)
    step = m * lax.rsqrt(v + 1e-8) + 0.1 * w
    return (w - 0.02 * step).astype(BF16), m, v


def stepped(me, squares, count, unit, g, w, m, v, before):
    layer, start, rows = unit
    whole, lanes = g.shape[1:]
    n = rows // 5
    here = pl.BlockSpec((1, n, lanes), lambda i, me: (layer, start // n + i, 0))
    specs = [
        pl.BlockSpec((8, 128), lambda i, me: (0, 0)),
        here,
        pl.BlockSpec((1, n, lanes), lambda i, me: (layer, me[0] * (whole // n) + start // n + i, 0)),
        here,
        here,
    ]
    moment = jax.ShapeDtypeStruct(m.shape, F32)
    return pl.pallas_call(
        functools.partial(step_kernel, count, True),
        out_shape=[jax.ShapeDtypeStruct((rows, lanes), BF16), moment, moment],
        grid_spec=pltpu.PrefetchScalarGridSpec(
            num_scalar_prefetch=1,
            grid=(rows // n,),
            in_specs=specs + [pl.BlockSpec(memory_space=pl.ANY)] * len(before),
            out_specs=[pl.BlockSpec((n, lanes), lambda i, me: (i, 0)), here, here],
        ),
        input_output_aliases={6 + i: 1 + i for i in range(len(before))},
        cost_estimate=pl.CostEstimate(flops=15 * rows * lanes, bytes_accessed=22 * rows * lanes, transcendentals=rows * lanes),
        name="adamw",
    )(me, squares, g, w, m, v, *before)


def place_kernel(places, n_before, in_vmem, *refs):
    n = len(places)
    blocks, out = refs[:n], refs[n + n_before]
    out_sem, refs = refs[n + n_before + 1], refs[n + n_before + 2 :]
    loads = []
    if not in_vmem:
        held, in_sem = refs[:n], refs[n]
        loads = [pltpu.make_async_copy(b, h, in_sem.at[i]) for i, (b, h) in enumerate(zip(blocks, held))]
        blocks = held
    for one in loads:
        one.start()
    stores = []
    for i, (offset, layer, start) in enumerate(places):
        if loads:
            loads[i].wait()
        at = pl.multiple_of(place(*offset) * (out.shape[1] // 8) + start, 16)
        stores.append(pltpu.make_async_copy(blocks[i], out.at[layer, pl.ds(at, blocks[i].shape[0])], out_sem.at[i]))
        stores[-1].start()
    for one in stores:
        one.wait()


def placed(blocks, places, shape, before, in_vmem=False):
    n = len(blocks)
    any_ = pl.BlockSpec(memory_space=pl.ANY)
    scratch = [pltpu.SemaphoreType.DMA((n,))]
    if not in_vmem:
        scratch += [pltpu.VMEM(b.shape, BF16) for b in blocks] + [pltpu.SemaphoreType.DMA((n,))]
    return pl.pallas_call(
        functools.partial(place_kernel, places, len(before), in_vmem),
        out_shape=jax.ShapeDtypeStruct(shape, BF16),
        in_specs=[pl.BlockSpec(memory_space=pltpu.VMEM) if in_vmem else any_] * n + [any_] * len(before),
        out_specs=any_,
        scratch_shapes=scratch,
        input_output_aliases={n: 0} if before else {},
        compiler_params=pltpu.CompilerParams(vmem_limit_bytes=16 * 1024 * 1024) if in_vmem else None,
        cost_estimate=pl.CostEstimate(flops=0, bytes_accessed=4 * sum(b.size for b in blocks), transcendentals=0),
        name="place",
    )(*blocks, *before)


def send(block, dx=0, dy=0, dc=0):
    flip = 4 * dx + 2 * dy + dc
    return lax.ppermute(block, "dp", [(d, d ^ flip) for d in range(8)])


def parts_of(layers, shapes):
    units = []
    for a, (rows, _) in enumerate(shapes):
        for l in range(layers):
            cuts = 2 if (a, l) == (0, 0) else 4 if (a, l) == (2, layers - 1) else 1
            units += [(a, l, i * rows // cuts, rows // cuts) for i in range(cuts)]
    return units


def solution(mesh):
    layers, shapes = 2, [(160, 5120), (160, 5120), (640, 1280)]
    units = parts_of(layers, shapes)
    groups = []
    for i, (a, l, _, rows) in enumerate(units):
        if groups and len(groups[-1]) == 1 and units[i - 1][:2] == (a, l):
            groups[-1].append(i)
        else:
            groups.append([i])

    def step(*arrays):
        terms, weights, m, v = (arrays[i : i + 3] for i in (0, 3, 6, 9))
        gradients, squares = summed(terms)
        count = 8 * sum(g.size for g in gradients)
        me = lax.axis_index("dp")[None]
        new_m, new_v, whole = [()] * 3, [()] * 3, [()] * 3
        first, second = [], []
        for a, *unit in units:
            before = (new_m[a], new_v[a]) if len(new_m[a]) else ()
            own, new_m[a], new_v[a] = stepped(me, squares, count, unit, gradients[a], weights[a], m[a], v[a], before)
            first.append((own, send(own, dx=1), send(own, dy=1), send(own, dc=1)))
        for i, (own, x, y, c) in enumerate(first):
            far = send(y, dx=1) if i % 2 else send(x, dy=1)
            second.append((far, send(x, dc=1), send(y, dc=1)))
        for i, (a, l, start, _) in enumerate(units):
            own, x, y, c = first[i]
            far, xc, yc = second[i]
            places = [(at, l, start) for at in ((0, 0, 0), (1, 0, 0), (0, 1, 0), (0, 0, 1), (1, 0, 1), (0, 1, 1))]
            whole[a] = placed([own, x, y, c, xc, yc], places, weights[a].shape, (whole[a],) if len(whole[a]) else ())
        for group in groups:
            blocks, places = [], []
            for i in group:
                a, l, start, _ = units[i]
                far = second[i][0]
                blocks += [far, send(far, dc=1)]
                places += [((1, 1, 0), l, start), ((1, 1, 1), l, start)]
            whole[a] = placed(blocks, places, weights[a].shape, (whole[a],), in_vmem=True)
        return (*whole, *new_m, *new_v)

    all_of, cut = P(None, None, None), P(None, "dp", None)
    return jax.shard_map(
        step,
        mesh=mesh,
        in_specs=(P(("rep", "dp"), None, None, None),) * 3 + (all_of,) * 3 + (cut,) * 6,
        out_specs=(P("rep", None, None),) * 3 + (P("rep", "dp", None),) * 6,
        check_vma=False,
    )
```

```python
import functools

import jax
import jax.numpy as jnp
from jax import lax
from jax.experimental import pallas as pl
from jax.experimental.pallas import tpu as pltpu
from jax.sharding import PartitionSpec as P


MESH = pl.DeviceIdType.MESH
F32, BF16 = jnp.float32, jnp.bfloat16
CHIPS = ((1, 1), (1, 0), (0, 1), (0, 0))


def place(dx=0, dy=0, dc=0):
    me = lax.axis_index("dp")
    x, y, c = me // 4, lax.rem(me // 2, 2), lax.rem(me, 2)
    x = 1 - x if dx else x
    y = 1 - y if dy else y
    c = 1 - c if dc else c
    return 4 * x + 2 * y + c


def add_into(dst, parts):
    def body(i, carry):
        s = pl.ds(pl.multiple_of(i * 16, 16), 16)
        total = parts[0][s, :].astype(F32)
        for p in parts[1:]:
            total = total + p[s, :].astype(F32)
        dst[s, :] = total.astype(BF16)
        return carry

    lax.fori_loop(0, dst.shape[0] // 16, body, 0)


def add_square(dst, parts, lanes, acc):
    def body(i, carry):
        s = pl.ds(pl.multiple_of(i * 16, 16), 16)
        total = parts[0][s, :].astype(F32)
        for p in parts[1:]:
            total = total + p[s, :].astype(F32)
        total = total.astype(BF16)
        dst[s, :] = total
        total = total.astype(F32)
        for k in range(lanes // 128):
            one = total[:, k * 128 : (k + 1) * 128]
            carry = carry + one * one
        return carry

    acc[...] += lax.fori_loop(0, dst.shape[0] // 16, body, jnp.zeros((16, 128), F32))


def sum_kernel(shapes, count, head, *refs):
    g, (w0, m0, v0), refs = refs[:3], refs[3:6], refs[6:]
    out, squares, new0, refs = refs[:3], refs[3], refs[4], refs[5:]
    near, refs = refs[:3], refs[3:]
    snd, rcv, own, par, refs = refs[0:2], refs[2:4], refs[4:6], refs[6:8], refs[8:]
    first, refs = refs[:4], refs[4:]
    acc, norms, d2d_s, d2d_r, link_s, link_r, own_sem, par_sem, out_sem, norm_s, norm_r, first_sem = refs
    layers = g[0].shape[1]
    units = [(a, l) for a in range(3) for l in range(layers)]
    end = len(units) - 1
    kind = [0, 0, 1]
    slot = {}
    for a, l in units:
        slot[a, l] = sum(1 for u in slot if kind[u[0]] == kind[a])
    me = lax.axis_index("dp")
    rep = lax.axis_index("rep")
    xn, yn, cn = place(dx=1), place(dy=1), place(dc=1)

    barrier = pltpu.get_barrier_semaphore()
    others = [lax.rem(me + k, 8) for k in range(1, 8)]
    for d in others:
        pl.semaphore_signal(barrier, inc=1, device_id=(rep, d), device_id_type=MESH)

    mine = pl.ds(pl.multiple_of(me * shapes[0][0], 16), head)
    ahead = [
        pltpu.make_async_copy(w0.at[0, mine], first[0], first_sem.at[0]),
        pltpu.make_async_copy(m0.at[0, pl.ds(0, head)], first[1], first_sem.at[1]),
        pltpu.make_async_copy(v0.at[0, pl.ds(0, head)], first[2], first_sem.at[2]),
    ]

    def split(i, j):
        n = shapes[units[i][0]][0] // 2
        if i == 0 and j < 2:
            return [(0, 16), (16, n - 16)]
        if i == end and j >= 4:
            return [(0, n - n // 5), (n - n // 5, n // 5)]
        return [(0, n)]

    d2d = {}

    def cut(s, h):
        return {(0, 0): 0, (0, 1): 1, (1, 0): 2, (2, 1): 3, (1, 1): 4, (2, 0): 5}.get((s, h))

    def rows(u, device, h, piece):
        a, l = u
        n = shapes[a][0] // 2
        return g[a].at[0, l, pl.ds(pl.multiple_of(device * (2 * n) + h * n + piece[0], 16), piece[1])]

    sends = []
    for i, u in enumerate(units):
        n = shapes[u[0]][0] // 2
        halves = [(s, h) for s in range(4) for h in range(2)]
        todo = [(s, h, p) for s, h in halves for p in (split(i, cut(s, h)) if i == 0 and s == 0 else [(0, n)])]
        if i == 0:
            todo.sort(key=lambda one: one[2] != (0, 16))
        sends += [(i, *one) for one in todo]
    for k, (i, s, h, p) in enumerate(sends):
        a, l = units[i]
        d2d[i, s, h, p] = pltpu.make_async_remote_copy(
            src_ref=rows(units[i], place(*CHIPS[s], 1), h, p),
            dst_ref=near[a].at[l, s, h, pl.ds(*p)],
            send_sem=d2d_s.at[k],
            recv_sem=d2d_r.at[k],
            device_id=(rep, cn),
            device_id_type=MESH,
        )

    tasks = []
    for i in range(end + 1):
        both = [(i, s, h, p, (), j) for j, s, h in ((0, 0, 0), (1, 0, 1)) for p in split(i, j)]
        both.sort(key=lambda one: one[3][0])
        tasks += both + [(i, s, h, p, (), j) for j, s, h in ((2, 1, 0), (3, 2, 1)) for p in split(i, j)]
    for i in range(end + 1):
        for p4, p5 in zip(split(i, 4), split(i, 5)):
            tasks += [(i, 1, 1, p4, (1,), 4), (i, 2, 0, p5, (0,), 5)]
    for i in range(end + 1):
        for p4, p5 in zip(split(i, 4), split(i, 5)):
            tasks += [(i, 3, 0, p5, (2, 5), None), (i, 3, 1, p4, (3, 4), None)]

    numbers = {key: k for k, key in enumerate((i, j, p) for i in range(end + 1) for j in range(6) for p in split(i, j))}

    def link(i, j, p):
        a, l = units[i]
        k = kind[a]
        return pltpu.make_async_remote_copy(
            src_ref=snd[k].at[slot[a, l], j % 4, pl.ds(*p)],
            dst_ref=rcv[k].at[slot[a, l], j, pl.ds(*p)],
            send_sem=link_s.at[numbers[i, j, p]],
            recv_sem=link_r.at[numbers[i, j, p]],
            device_id=(rep, xn if j % 2 == 0 else yn),
            device_id_type=MESH,
        )

    done = set()

    def once(what, wait):
        if what not in done:
            done.add(what)
            wait()

    def arrived(i, j, piece):
        for p in split(i, j):
            if p[0] < piece[0] + piece[1] and piece[0] < p[0] + p[1]:
                once(("arrived", i, j, p), lambda: link(i, j, p).wait_recv())

    def left(i, j):
        for p in split(i, j):
            once(("left", i, j, p), lambda: link(i, j, p).wait_send())

    loads = {}

    def load_mine(t):
        i, s, h, p, _, _ = tasks[t]
        k, b = kind[units[i][0]], t % 2
        loads[t] = [pltpu.make_async_copy(rows(units[i], place(*CHIPS[s], 0), h, p), own[k].at[b, pl.ds(0, p[1])], own_sem.at[b])]
        loads[t][0].start()

    def load_theirs(t):
        i, s, h, p, _, _ = tasks[t]
        a, l = units[i]
        k, b = kind[a], t % 2
        whole = p if (i, s, h, p) in d2d else (0, shapes[a][0] // 2)
        once(("near", i, s, h, whole), d2d[i, s, h, whole].wait_recv)
        loads[t] += [pltpu.make_async_copy(near[a].at[l, s, h, pl.ds(*p)], par[k].at[b, pl.ds(0, p[1])], par_sem.at[b])]
        loads[t][1].start()

    load_mine(0)
    acc[...] = jnp.zeros_like(acc)
    pl.semaphore_wait(barrier, 7)
    for one in d2d.values():
        one.start()
    for one in ahead:
        one.start()
    load_theirs(0)
    stores = []
    for t, (i, s, h, p, added, j) in enumerate(tasks):
        if t + 1 < len(tasks):
            load_mine(t + 1)
            load_theirs(t + 1)
        a, l = units[i]
        k = kind[a]
        for one in loads[t]:
            one.wait()
        for r in added:
            arrived(i, r, p)
        parts = [own[k].at[t % 2, pl.ds(0, p[1])], par[k].at[t % 2, pl.ds(0, p[1])]]
        parts += [rcv[k].at[slot[a, l], r, pl.ds(*p)] for r in added]
        if j is None:
            dst = snd[k].at[slot[a, l], 2 + h, pl.ds(*p)]
            left(i, 2 + h)
            add_square(dst, parts, shapes[a][1], acc)
            store = pltpu.make_async_copy(dst, out[a].at[l, pl.ds(h * (shapes[a][0] // 2) + p[0], p[1])], out_sem.at[len(stores)])
            store.start()
            stores.append(store)
        else:
            dst = snd[k].at[slot[a, l], j % 4, pl.ds(*p)]
            if j >= 4:
                left(i, j - 4)
            add_into(dst, parts)
            link(i, j, p).start()

    sent = []
    for k in range(1, 8):
        to = lax.rem(me + k, 8)
        copy = pltpu.make_async_remote_copy(
            src_ref=acc, dst_ref=norms.at[me], send_sem=norm_s.at[k - 1], recv_sem=norm_r.at[k - 1], device_id=(rep, to), device_id_type=MESH
        )
        copy.start()
        sent.append(copy)
    norms[me] = acc[...]
    for one in ahead:
        one.wait()
    for store in stores:
        store.wait()
    for copy in d2d.values():
        copy.wait_send()
    for i in range(end + 1):
        for j in range(6):
            left(i, j)
    for copy in sent:
        copy.wait_recv()
    total = norms[0]
    for d in range(1, 8):
        total = total + norms[d]
    total = jnp.sum(total, axis=0, keepdims=True)
    total = jnp.sum(total, axis=1, keepdims=True)
    squares[...] = jnp.broadcast_to(total, squares.shape)

    half = snd[0].at[slot[0, 0], 2]

    def body(i, carry):
        r = pl.ds(pl.multiple_of(i * 16, 16), 16)
        first[3][r, :] = stepped_block(total, count, half[r, :], first[0][r, :], first[1][r, :], first[2][r, :])[0]
        return carry

    lax.fori_loop(0, head // 16, body, 0)
    last = pltpu.make_async_copy(first[3], new0, first_sem.at[3])
    last.start()
    for copy in sent:
        copy.wait_send()
    last.wait()


def summed(terms, count, head, w, m, v):
    layers = terms[0].shape[1]
    shapes = [(t.shape[2] // 8, t.shape[3]) for t in terms]
    halves = [(shapes[0][0] // 2, shapes[0][1]), (shapes[2][0] // 2, shapes[2][1])]
    counts = [2 * layers, layers]
    any_ = pl.BlockSpec(memory_space=pl.ANY)
    outs = pl.pallas_call(
        functools.partial(sum_kernel, shapes, count, head),
        out_shape=[jax.ShapeDtypeStruct((layers, *s), BF16) for s in shapes]
        + [jax.ShapeDtypeStruct((8, 128), F32)]
        + [jax.ShapeDtypeStruct((head, shapes[0][1]), BF16)]
        + [jax.ShapeDtypeStruct((layers, 4, 2, s[0] // 2, s[1]), BF16) for s in shapes],
        in_specs=[any_] * 6,
        out_specs=[any_] * 3 + [pl.BlockSpec(memory_space=pltpu.VMEM)] + [any_] * 4,
        scratch_shapes=[pltpu.VMEM((n, 4, *s), BF16) for n, s in zip(counts, halves)]
        + [pltpu.VMEM((n, 6, *s), BF16) for n, s in zip(counts, halves)]
        + [pltpu.VMEM((2, *s), BF16) for s in halves] * 2
        + [pltpu.VMEM((head, shapes[0][1]), t) for t in (BF16, F32, F32, BF16)]
        + [
            pltpu.VMEM((16, 128), F32),
            pltpu.VMEM((8, 16, 128), F32),
            pltpu.SemaphoreType.DMA((24 * layers + 2,)),
            pltpu.SemaphoreType.DMA((24 * layers + 2,)),
            pltpu.SemaphoreType.DMA((18 * layers + 4,)),
            pltpu.SemaphoreType.DMA((18 * layers + 4,)),
            pltpu.SemaphoreType.DMA((2,)),
            pltpu.SemaphoreType.DMA((2,)),
            pltpu.SemaphoreType.DMA((6 * layers + 2,)),
            pltpu.SemaphoreType.DMA((7,)),
            pltpu.SemaphoreType.DMA((7,)),
            pltpu.SemaphoreType.DMA((4,)),
        ],
        compiler_params=pltpu.CompilerParams(collective_id=0, has_side_effects=True, vmem_limit_bytes=62 * 1024 * 1024),
        name="sum_terms",
    )(*terms, w, m, v)
    return outs[:3], outs[3], outs[4]


def step_kernel(count, with_weight, me, squares, g, w, m, v, *rest):
    new = stepped_block(squares[:1, :1], count, g[0], w[0], m[0], v[0])
    rest[-2][0], rest[-1][0] = new[1:]
    if with_weight:
        rest[-3][...] = new[0]


def stepped_block(squares, count, g, w, m, v):
    g = g.astype(F32) * jnp.minimum(1.0, 0.5 * lax.rsqrt(squares / count + 1e-30))
    m = 0.9 * m + 0.1 * g
    v = 0.95 * v + 0.05 * g * g
    w = w.astype(F32)
    step = m * lax.rsqrt(v + 1e-8) + 0.1 * w
    return (w - 0.02 * step).astype(BF16), m, v


def stepped(me, squares, count, unit, g, w, m, v, before, with_weight):
    layer, start, rows = unit
    whole, lanes = g.shape[1:]
    n = rows // 5
    here = pl.BlockSpec((1, n, lanes), lambda i, me: (layer, start // n + i, 0))
    specs = [
        pl.BlockSpec((8, 128), lambda i, me: (0, 0)),
        here,
        pl.BlockSpec((1, n, lanes), lambda i, me: (layer, me[0] * (whole // n) + start // n + i, 0)),
        here,
        here,
    ]
    moment = jax.ShapeDtypeStruct(m.shape, F32)
    return pl.pallas_call(
        functools.partial(step_kernel, count, with_weight),
        out_shape=[jax.ShapeDtypeStruct((rows, lanes), BF16)] * with_weight + [moment, moment],
        grid_spec=pltpu.PrefetchScalarGridSpec(
            num_scalar_prefetch=1,
            grid=(rows // n,),
            in_specs=specs + [pl.BlockSpec(memory_space=pl.ANY)] * len(before),
            out_specs=[pl.BlockSpec((n, lanes), lambda i, me: (i, 0))] * with_weight + [here, here],
        ),
        input_output_aliases={6 + i: with_weight + i for i in range(len(before))},
        cost_estimate=pl.CostEstimate(flops=15 * rows * lanes, bytes_accessed=22 * rows * lanes, transcendentals=rows * lanes),
        name="adamw",
    )(me, squares, g, w, m, v, *before)


def place_kernel(places, n_before, in_vmem, *refs):
    n = len(places)
    blocks, out = refs[:n], refs[n + n_before]
    out_sem, refs = refs[n + n_before + 1], refs[n + n_before + 2 :]
    loads = []
    if not in_vmem:
        held, in_sem = refs[:n], refs[n]
        loads = [pltpu.make_async_copy(b, h, in_sem.at[i]) for i, (b, h) in enumerate(zip(blocks, held))]
        blocks = held
    for one in loads:
        one.start()
    stores = []
    for i, (offset, layer, start) in enumerate(places):
        if loads:
            loads[i].wait()
        at = pl.multiple_of(place(*offset) * (out.shape[1] // 8) + start, 16)
        stores.append(pltpu.make_async_copy(blocks[i], out.at[layer, pl.ds(at, blocks[i].shape[0])], out_sem.at[i]))
        stores[-1].start()
    for one in stores:
        one.wait()


def placed(blocks, places, shape, before, in_vmem=False):
    n = len(blocks)
    any_ = pl.BlockSpec(memory_space=pl.ANY)
    scratch = [pltpu.SemaphoreType.DMA((n,))]
    if not in_vmem:
        scratch += [pltpu.VMEM(b.shape, BF16) for b in blocks] + [pltpu.SemaphoreType.DMA((n,))]
    return pl.pallas_call(
        functools.partial(place_kernel, places, len(before), in_vmem),
        out_shape=jax.ShapeDtypeStruct(shape, BF16),
        in_specs=[pl.BlockSpec(memory_space=pltpu.VMEM) if in_vmem else any_] * n + [any_] * len(before),
        out_specs=any_,
        scratch_shapes=scratch,
        input_output_aliases={n: 0} if before else {},
        compiler_params=pltpu.CompilerParams(vmem_limit_bytes=16 * 1024 * 1024) if in_vmem else None,
        cost_estimate=pl.CostEstimate(flops=0, bytes_accessed=4 * sum(b.size for b in blocks), transcendentals=0),
        name="place",
    )(*blocks, *before)


def send(block, dx=0, dy=0, dc=0):
    flip = 4 * dx + 2 * dy + dc
    return lax.ppermute(block, "dp", [(d, d ^ flip) for d in range(8)])


def parts_of(layers, shapes):
    units = []
    for a, (rows, _) in enumerate(shapes):
        for l in range(layers):
            cuts = 2 if (a, l) == (0, 0) else 4 if (a, l) == (2, layers - 1) else 1
            units += [(a, l, i * rows // cuts, rows // cuts) for i in range(cuts)]
    return units


def solution(mesh):
    layers, shapes = 2, [(160, 5120), (160, 5120), (640, 1280)]
    units = parts_of(layers, shapes)
    groups = []
    for i, (a, l, _, rows) in enumerate(units):
        if groups and len(groups[-1]) == 1 and units[i - 1][:2] == (a, l):
            groups[-1].append(i)
        else:
            groups.append([i])

    def step(*arrays):
        terms, weights, m, v = (arrays[i : i + 3] for i in (0, 3, 6, 9))
        count = 8 * sum(one.size for one in m)
        gradients, squares, head = summed(terms, count, units[0][3], weights[0], m[0], v[0])
        me = lax.axis_index("dp")[None]
        new_m, new_v, whole = [()] * 3, [()] * 3, [()] * 3
        first, second = [], []
        for i, (a, *unit) in enumerate(units):
            before = (new_m[a], new_v[a]) if len(new_m[a]) else ()
            *own, new_m[a], new_v[a] = stepped(me, squares, count, unit, gradients[a], weights[a], m[a], v[a], before, i > 0)
            own = own[0] if own else head
            first.append((own, send(own, dx=1), send(own, dy=1), send(own, dc=1)))
        for i, (own, x, y, c) in enumerate(first):
            far = send(y, dx=1) if i % 2 else send(x, dy=1)
            second.append((far, send(x, dc=1), send(y, dc=1)))
        for i, (a, l, start, _) in enumerate(units):
            own, x, y, c = first[i]
            far, xc, yc = second[i]
            places = [(at, l, start) for at in ((0, 0, 0), (1, 0, 0), (0, 1, 0), (0, 0, 1), (1, 0, 1), (0, 1, 1))]
            whole[a] = placed([own, x, y, c, xc, yc], places, weights[a].shape, (whole[a],) if len(whole[a]) else ())
        for group in groups:
            blocks, places = [], []
            for i in group:
                a, l, start, _ = units[i]
                far = second[i][0]
                blocks += [far, send(far, dc=1)]
                places += [((1, 1, 0), l, start), ((1, 1, 1), l, start)]
            whole[a] = placed(blocks, places, weights[a].shape, (whole[a],), in_vmem=True)
        return (*whole, *new_m, *new_v)

    all_of, cut = P(None, None, None), P(None, "dp", None)
    return jax.shard_map(
        step,
        mesh=mesh,
        in_specs=(P(("rep", "dp"), None, None, None),) * 3 + (all_of,) * 3 + (cut,) * 6,
        out_specs=(P("rep", None, None),) * 3 + (P("rep", "dp", None),) * 6,
        check_vma=False,
    )
```

```python
import functools

import jax
import jax.numpy as jnp
from jax import lax
from jax.experimental import pallas as pl
from jax.experimental.pallas import tpu as pltpu
from jax.sharding import PartitionSpec as P


MESH = pl.DeviceIdType.MESH
F32, BF16 = jnp.float32, jnp.bfloat16
CHIPS = ((1, 1), (1, 0), (0, 1), (0, 0))


def place(dx=0, dy=0, dc=0):
    me = lax.axis_index("dp")
    x, y, c = me // 4, lax.rem(me // 2, 2), lax.rem(me, 2)
    x = 1 - x if dx else x
    y = 1 - y if dy else y
    c = 1 - c if dc else c
    return 4 * x + 2 * y + c


def add_into(dst, parts):
    def body(i, carry):
        s = pl.ds(pl.multiple_of(i * 16, 16), 16)
        total = parts[0][s, :].astype(F32)
        for p in parts[1:]:
            total = total + p[s, :].astype(F32)
        dst[s, :] = total.astype(BF16)
        return carry

    lax.fori_loop(0, dst.shape[0] // 16, body, 0)


def add_square(dst, parts, lanes, acc):
    def body(i, carry):
        s = pl.ds(pl.multiple_of(i * 16, 16), 16)
        total = parts[0][s, :].astype(F32)
        for p in parts[1:]:
            total = total + p[s, :].astype(F32)
        total = total.astype(BF16)
        dst[s, :] = total
        total = total.astype(F32)
        for k in range(lanes // 128):
            one = total[:, k * 128 : (k + 1) * 128]
            carry = carry + one * one
        return carry

    acc[...] += lax.fori_loop(0, dst.shape[0] // 16, body, jnp.zeros((16, 128), F32))


def sum_kernel(shapes, count, head, *refs):
    g, (w0, m0, v0), refs = refs[:3], refs[3:6], refs[6:]
    out, squares, new0, refs = refs[:3], refs[3], refs[4], refs[5:]
    near, refs = refs[:3], refs[3:]
    snd, rcv, own, par, refs = refs[0:2], refs[2:4], refs[4:6], refs[6:8], refs[8:]
    first, early, refs = refs[:4], refs[4], refs[5:]
    acc, norms, d2d_s, d2d_r, link_s, link_r, own_sem, par_sem, out_sem, norm_s, norm_r, first_sem, early_sem, ready = refs
    layers = g[0].shape[1]
    units = [(a, l) for a in range(3) for l in range(layers)]
    end = len(units) - 1
    kind = [0, 0, 1]
    slot = {}
    for a, l in units:
        slot[a, l] = sum(1 for u in slot if kind[u[0]] == kind[a])
    me = lax.axis_index("dp")
    rep = lax.axis_index("rep")
    xn, yn, cn = place(dx=1), place(dy=1), place(dc=1)

    barrier = pltpu.get_barrier_semaphore()

    def tell(sem):
        for d in (cn, xn, yn):
            pl.semaphore_signal(sem, inc=1, device_id=(rep, d), device_id_type=MESH)

    tell(barrier)

    mine = pl.ds(pl.multiple_of(me * shapes[0][0], 16), head)
    ahead = [
        pltpu.make_async_copy(w0.at[0, mine], first[0], first_sem.at[0]),
        pltpu.make_async_copy(m0.at[0, pl.ds(0, head)], first[1], first_sem.at[1]),
        pltpu.make_async_copy(v0.at[0, pl.ds(0, head)], first[2], first_sem.at[2]),
    ]

    def split(i, j):
        n = shapes[units[i][0]][0] // 2
        if i == 0 and j < 2:
            return [(0, 16), (16, n - 16)]
        if i == end and j >= 4:
            return [(0, n - n // 5), (n - n // 5, n // 5)]
        return [(0, n)]

    def rows(u, device, h, piece):
        a, l = u
        n = shapes[a][0] // 2
        return g[a].at[0, l, pl.ds(pl.multiple_of(device * (2 * n) + h * n + piece[0], 16), piece[1])]

    def all_of(ref, sem):
        pltpu.make_async_copy(ref, ref, sem).wait()

    opening = [(0, h, p) for p in split(0, 0) for h in range(2)]
    near_sends = []
    for k, (s, h, p) in enumerate(opening):
        near_sends.append((early.at[h] if k < 2 else rows(units[0], place(*CHIPS[s], 1), h, p), par[0].at[h, pl.ds(*p)], 0, k))
    for i, (a, l) in enumerate(units):
        for s in range(4):
            if (i, s) != (0, 0):
                near_sends.append((rows(units[i], place(*CHIPS[s], 1), 0, (0, shapes[a][0])), near[a].at[l, s], a, 4 + i))
    near_sends = [
        pltpu.make_async_remote_copy(
            src_ref=src, dst_ref=dst, send_sem=d2d_s.at[a], recv_sem=d2d_r.at[k], device_id=(rep, cn), device_id_type=MESH
        )
        for src, dst, a, k in near_sends
    ]

    tasks = []
    for i in range(end + 1):
        both = [(i, s, h, p, (), j) for j, s, h in ((0, 0, 0), (1, 0, 1)) for p in split(i, j)]
        both.sort(key=lambda one: one[3][0])
        tasks += both + [(i, s, h, p, (), j) for j, s, h in ((2, 1, 0), (3, 2, 1)) for p in split(i, j)]
    for i in range(end + 1):
        for p4, p5 in zip(split(i, 4), split(i, 5)):
            tasks += [(i, 1, 1, p4, (1,), 4), (i, 2, 0, p5, (0,), 5)]
    for i in range(end + 1):
        for p4, p5 in zip(split(i, 4), split(i, 5)):
            tasks += [(i, 3, 0, p5, (2, 5), None), (i, 3, 1, p4, (3, 4), None)]

    def arrival(i, j, p):
        return link_r.at[3 * len(units) if j >= 4 and i == end and p[0] else 3 * i + j // 2]

    def link(i, j, p):
        a, l = units[i]
        k = kind[a]
        return pltpu.make_async_remote_copy(
            src_ref=snd[k].at[slot[a, l], j % 4, pl.ds(*p)],
            dst_ref=rcv[k].at[slot[a, l], j, pl.ds(*p)],
            send_sem=link_s.at[j // 4, i],
            recv_sem=arrival(i, j, p),
            device_id=(rep, xn if j % 2 == 0 else yn),
            device_id_type=MESH,
        )

    done = set()

    def once(what, wait):
        if what not in done:
            done.add(what)
            wait()

    def arrived(i, j, p):
        a, l = units[i]
        into = rcv[kind[a]].at[slot[a, l], pl.ds(j - j % 2, 2)]
        if j >= 4:
            into = into.at[:, pl.ds(*p)]
            once(("arrived", i, 4, p), lambda: all_of(into, arrival(i, j, p)))
        else:
            once(("arrived", i, j // 2), lambda: all_of(into, arrival(i, j, p)))

    def left(i):
        a, l = units[i]
        once(("left", i), lambda: all_of(snd[kind[a]].at[slot[a, l]], link_s.at[0, i]))

    loads = {}

    def load_mine(t):
        i, s, h, p, _, _ = tasks[t]
        k, b = kind[units[i][0]], t % 2
        at = pl.ds(*p) if t < 4 else pl.ds(0, p[1])
        loads[t] = [pltpu.make_async_copy(rows(units[i], place(*CHIPS[s], 0), h, p), own[k].at[b, at], own_sem.at[t if t < 4 else b])]
        loads[t][0].start()

    def load_theirs(t):
        i, s, h, p, _, _ = tasks[t]
        a, l = units[i]
        k, b = kind[a], t % 2
        all_near = near[a].at[l] if i else near[a].at[l, pl.ds(1, 3)]
        once(("near", i), lambda: all_of(all_near, d2d_r.at[4 + i]))
        at = pl.ds(h * (shapes[a][0] // 2) + p[0], p[1])
        loads[t] += [pltpu.make_async_copy(near[a].at[l, s, at], par[k].at[b, pl.ds(0, p[1])], par_sem.at[b])]
        loads[t][1].start()

    taken = [pltpu.make_async_copy(rows(units[0], place(*CHIPS[0], 1), h, (0, 16)), early.at[h], early_sem.at[0]) for h in range(2)]
    for one in taken:
        one.start()
    for t in range(4):
        load_mine(t)
    acc[...] = jnp.zeros_like(acc)
    all_of(early, early_sem.at[0])
    pl.semaphore_wait(barrier, 3)
    for one in near_sends[:4]:
        one.start()
    for t, (i, s, h, p, added, j) in enumerate(tasks):
        if t == 2:
            for one in near_sends[4:]:
                one.start()
            tell(ready.at[0])
        if t == 12:
            for one in ahead:
                one.start()
        here = t > 3 and t + 1 < len(tasks) and ("near", tasks[t + 1][0]) in done
        late = t > 2 and t + 1 < len(tasks) and not here
        if here:
            load_mine(t + 1)
            load_theirs(t + 1)
        if t in (8, 16):
            pl.semaphore_wait(ready.at[t // 8 - 1], 3)
            if t == 8:
                tell(ready.at[1])
        a, l = units[i]
        k = kind[a]
        for one in loads[t]:
            one.wait()
        if t < 4:
            near_sends[t].wait_recv()
        for r in added:
            arrived(i, r, p)
        held = pl.ds(p[0] if t < 4 else 0, p[1])
        parts = [own[k].at[t % 2, held], par[k].at[t % 2, held]]
        parts += [rcv[k].at[slot[a, l], r, pl.ds(*p)] for r in added]
        if j is None:
            dst = snd[k].at[slot[a, l], 2 + h, pl.ds(*p)]
            left(i)
            add_square(dst, parts, shapes[a][1], acc)
            store = pltpu.make_async_copy(dst, out[a].at[l, pl.ds(h * (shapes[a][0] // 2) + p[0], p[1])], out_sem.at[a])
            store.start()
        else:
            dst = snd[k].at[slot[a, l], j % 4, pl.ds(*p)]
            if j >= 4:
                left(i)
            add_into(dst, parts)
            link(i, j, p).start()
        if late:
            load_mine(t + 1)
            load_theirs(t + 1)

    for k in range(1, 8):
        pltpu.make_async_remote_copy(
            src_ref=acc,
            dst_ref=norms.at[me],
            send_sem=norm_s.at[0],
            recv_sem=norm_r.at[0],
            device_id=(rep, lax.rem(me + k, 8)),
            device_id_type=MESH,
        ).start()
    norms[me] = acc[...]
    for one in ahead:
        one.wait()
    for a in range(3):
        all_of(out[a], out_sem.at[a])
        all_of(near[a], d2d_s.at[a])
    for i, (a, l) in enumerate(units):
        all_of(snd[kind[a]].at[slot[a, l], pl.ds(0, 2)], link_s.at[1, i])
    all_of(norms.at[pl.ds(0, 7)], norm_r.at[0])
    total = norms[0]
    for d in range(1, 8):
        total = total + norms[d]
    total = jnp.sum(total, axis=0, keepdims=True)
    total = jnp.sum(total, axis=1, keepdims=True)
    squares[...] = jnp.broadcast_to(total, squares.shape)

    half = snd[0].at[slot[0, 0], 2]

    for i in range(head // 16):
        r = pl.ds(i * 16, 16)
        first[3][r, :] = stepped_block(total, count, half[r, :], first[0][r, :], first[1][r, :], first[2][r, :])[0]
        pltpu.make_async_copy(first[3].at[r], new0.at[r], first_sem.at[3]).start()
    all_of(norms.at[pl.ds(0, 7)], norm_s.at[0])
    all_of(new0, first_sem.at[3])


def summed(terms, count, head, w, m, v):
    layers = terms[0].shape[1]
    shapes = [(t.shape[2] // 8, t.shape[3]) for t in terms]
    halves = [(shapes[0][0] // 2, shapes[0][1]), (shapes[2][0] // 2, shapes[2][1])]
    counts = [2 * layers, layers]
    any_ = pl.BlockSpec(memory_space=pl.ANY)
    outs = pl.pallas_call(
        functools.partial(sum_kernel, shapes, count, head),
        out_shape=[jax.ShapeDtypeStruct((layers, *s), BF16) for s in shapes]
        + [jax.ShapeDtypeStruct((8, 128), F32)]
        + [jax.ShapeDtypeStruct((head, shapes[0][1]), BF16)]
        + [jax.ShapeDtypeStruct((layers, 4, *s), BF16) for s in shapes],
        in_specs=[any_] * 6,
        out_specs=[any_] * 3 + [pl.BlockSpec(memory_space=pltpu.VMEM)] + [any_] * 4,
        scratch_shapes=[pltpu.VMEM((n, 4, *s), BF16) for n, s in zip(counts, halves)]
        + [pltpu.VMEM((n, 6, *s), BF16) for n, s in zip(counts, halves)]
        + [pltpu.VMEM((2, *s), BF16) for s in halves] * 2
        + [pltpu.VMEM((head, shapes[0][1]), t) for t in (BF16, F32, F32, BF16)]
        + [pltpu.VMEM((2, 16, shapes[0][1]), BF16)]
        + [
            pltpu.VMEM((16, 128), F32),
            pltpu.VMEM((8, 16, 128), F32),
            pltpu.SemaphoreType.DMA((3,)),
            pltpu.SemaphoreType.DMA((4 + 3 * layers,)),
            pltpu.SemaphoreType.DMA((2, 3 * layers)),
            pltpu.SemaphoreType.DMA((9 * layers + 1,)),
            pltpu.SemaphoreType.DMA((4,)),
            pltpu.SemaphoreType.DMA((2,)),
            pltpu.SemaphoreType.DMA((3,)),
            pltpu.SemaphoreType.DMA((1,)),
            pltpu.SemaphoreType.DMA((1,)),
            pltpu.SemaphoreType.DMA((4,)),
            pltpu.SemaphoreType.DMA((1,)),
            pltpu.SemaphoreType.REGULAR((2,)),
        ],
        compiler_params=pltpu.CompilerParams(collective_id=0, has_side_effects=True, vmem_limit_bytes=62 * 1024 * 1024),
        name="sum_terms",
    )(*terms, w, m, v)
    return outs[:3], outs[3], outs[4]


def step_kernel(count, with_weight, me, squares, g, w, m, v, *rest):
    new = stepped_block(squares[:1, :1], count, g[0], w[0], m[0], v[0])
    rest[-2][0], rest[-1][0] = new[1:]
    if with_weight:
        rest[-3][...] = new[0]


def stepped_block(squares, count, g, w, m, v):
    g = g.astype(F32) * jnp.minimum(1.0, 0.5 * lax.rsqrt(squares / count + 1e-30))
    m = 0.9 * m + 0.1 * g
    v = 0.95 * v + 0.05 * g * g
    w = w.astype(F32)
    step = m * lax.rsqrt(v + 1e-8) + 0.1 * w
    return (w - 0.02 * step).astype(BF16), m, v


def stepped(me, squares, count, unit, g, w, m, v, before, with_weight):
    layer, start, rows = unit
    whole, lanes = g.shape[1:]
    n = rows // 5
    here = pl.BlockSpec((1, n, lanes), lambda i, me: (layer, start // n + i, 0))
    specs = [
        pl.BlockSpec((8, 128), lambda i, me: (0, 0)),
        here,
        pl.BlockSpec((1, n, lanes), lambda i, me: (layer, me[0] * (whole // n) + start // n + i, 0)),
        here,
        here,
    ]
    moment = jax.ShapeDtypeStruct(m.shape, F32)
    return pl.pallas_call(
        functools.partial(step_kernel, count, with_weight),
        out_shape=[jax.ShapeDtypeStruct((rows, lanes), BF16)] * with_weight + [moment, moment],
        grid_spec=pltpu.PrefetchScalarGridSpec(
            num_scalar_prefetch=1,
            grid=(rows // n,),
            in_specs=specs + [pl.BlockSpec(memory_space=pl.ANY)] * len(before),
            out_specs=[pl.BlockSpec((n, lanes), lambda i, me: (i, 0))] * with_weight + [here, here],
        ),
        input_output_aliases={6 + i: with_weight + i for i in range(len(before))},
        cost_estimate=pl.CostEstimate(flops=15 * rows * lanes, bytes_accessed=22 * rows * lanes, transcendentals=rows * lanes),
        name="adamw",
    )(me, squares, g, w, m, v, *before)


def place_kernel(places, n_before, in_vmem, *refs):
    n = len(places)
    blocks, out = refs[:n], refs[n + n_before]
    out_sem, refs = refs[n + n_before + 1], refs[n + n_before + 2 :]
    loads = []
    if not in_vmem:
        held, in_sem = refs[:n], refs[n]
        loads = [pltpu.make_async_copy(b, h, in_sem.at[i]) for i, (b, h) in enumerate(zip(blocks, held))]
        blocks = held
    for one in loads:
        one.start()
    stores = []
    for i, (offset, layer, start) in enumerate(places):
        if loads:
            loads[i].wait()
        at = pl.multiple_of(place(*offset) * (out.shape[1] // 8) + start, 16)
        stores.append(pltpu.make_async_copy(blocks[i], out.at[layer, pl.ds(at, blocks[i].shape[0])], out_sem.at[i]))
        stores[-1].start()
    for one in stores:
        one.wait()


def placed(blocks, places, shape, before, in_vmem=False):
    n = len(blocks)
    any_ = pl.BlockSpec(memory_space=pl.ANY)
    scratch = [pltpu.SemaphoreType.DMA((n,))]
    if not in_vmem:
        scratch += [pltpu.VMEM(b.shape, BF16) for b in blocks] + [pltpu.SemaphoreType.DMA((n,))]
    return pl.pallas_call(
        functools.partial(place_kernel, places, len(before), in_vmem),
        out_shape=jax.ShapeDtypeStruct(shape, BF16),
        in_specs=[pl.BlockSpec(memory_space=pltpu.VMEM) if in_vmem else any_] * n + [any_] * len(before),
        out_specs=any_,
        scratch_shapes=scratch,
        input_output_aliases={n: 0} if before else {},
        compiler_params=pltpu.CompilerParams(vmem_limit_bytes=16 * 1024 * 1024) if in_vmem else None,
        cost_estimate=pl.CostEstimate(flops=0, bytes_accessed=4 * sum(b.size for b in blocks), transcendentals=0),
        name="place",
    )(*blocks, *before)


def send(block, dx=0, dy=0, dc=0):
    flip = 4 * dx + 2 * dy + dc
    return lax.ppermute(block, "dp", [(d, d ^ flip) for d in range(8)])


def parts_of(layers, shapes):
    units = []
    for a, (rows, _) in enumerate(shapes):
        for l in range(layers):
            cuts = 2 if (a, l) == (0, 0) else 4 if (a, l) == (2, layers - 1) else 1
            units += [(a, l, i * rows // cuts, rows // cuts) for i in range(cuts)]
    return units


def solution(mesh):
    layers, shapes = 2, [(160, 5120), (160, 5120), (640, 1280)]
    units = parts_of(layers, shapes)
    groups = []
    for i, (a, l, _, rows) in enumerate(units):
        if groups and len(groups[-1]) == 1 and units[i - 1][:2] == (a, l):
            groups[-1].append(i)
        else:
            groups.append([i])

    def step(*arrays):
        terms, weights, m, v = (arrays[i : i + 3] for i in (0, 3, 6, 9))
        count = 8 * sum(one.size for one in m)
        gradients, squares, head = summed(terms, count, units[0][3], weights[0], m[0], v[0])
        me = lax.axis_index("dp")[None]
        new_m, new_v, whole = [()] * 3, [()] * 3, [()] * 3
        first, second = [], []
        for i, (a, *unit) in enumerate(units):
            before = (new_m[a], new_v[a]) if len(new_m[a]) else ()
            *own, new_m[a], new_v[a] = stepped(me, squares, count, unit, gradients[a], weights[a], m[a], v[a], before, i > 0)
            own = own[0] if own else head
            first.append((own, send(own, dx=1), send(own, dy=1), send(own, dc=1)))
        for i, (own, x, y, c) in enumerate(first):
            far = send(y, dx=1) if i % 2 else send(x, dy=1)
            second.append((far, send(x, dc=1), send(y, dc=1)))
        for i, (a, l, start, _) in enumerate(units):
            own, x, y, c = first[i]
            far, xc, yc = second[i]
            places = [(at, l, start) for at in ((0, 0, 0), (1, 0, 0), (0, 1, 0), (0, 0, 1), (1, 0, 1), (0, 1, 1))]
            whole[a] = placed([own, x, y, c, xc, yc], places, weights[a].shape, (whole[a],) if len(whole[a]) else ())
        for group in groups:
            blocks, places = [], []
            for i in group:
                a, l, start, _ = units[i]
                far = second[i][0]
                blocks += [far, send(far, dc=1)]
                places += [((1, 1, 0), l, start), ((1, 1, 1), l, start)]
            whole[a] = placed(blocks, places, weights[a].shape, (whole[a],), in_vmem=True)
        return (*whole, *new_m, *new_v)

    all_of, cut = P(None, None, None), P(None, "dp", None)
    return jax.shard_map(
        step,
        mesh=mesh,
        in_specs=(P(("rep", "dp"), None, None, None),) * 3 + (all_of,) * 3 + (cut,) * 6,
        out_specs=(P("rep", None, None),) * 3 + (P("rep", "dp", None),) * 6,
        check_vma=False,
    )
```

```python
import functools

import jax
import jax.numpy as jnp
from jax import lax
from jax.experimental import pallas as pl
from jax.experimental.pallas import tpu as pltpu
from jax.sharding import PartitionSpec as P


MESH = pl.DeviceIdType.MESH
F32, BF16 = jnp.float32, jnp.bfloat16
CHIPS = ((1, 1), (1, 0), (0, 1), (0, 0))


def place(dx=0, dy=0, dc=0):
    me = lax.axis_index("dp")
    x, y, c = me // 4, lax.rem(me // 2, 2), lax.rem(me, 2)
    x = 1 - x if dx else x
    y = 1 - y if dy else y
    c = 1 - c if dc else c
    return 4 * x + 2 * y + c


def add_into(dst, parts):
    def body(i, carry):
        s = pl.ds(pl.multiple_of(i * 16, 16), 16)
        total = parts[0][s, :].astype(F32)
        for p in parts[1:]:
            total = total + p[s, :].astype(F32)
        dst[s, :] = total.astype(BF16)
        return carry

    lax.fori_loop(0, dst.shape[0] // 16, body, 0)


def add_square(dst, parts, lanes, acc):
    def body(i, carry):
        s = pl.ds(pl.multiple_of(i * 16, 16), 16)
        total = parts[0][s, :].astype(F32)
        for p in parts[1:]:
            total = total + p[s, :].astype(F32)
        total = total.astype(BF16)
        dst[s, :] = total
        total = total.astype(F32)
        for k in range(lanes // 128):
            one = total[:, k * 128 : (k + 1) * 128]
            carry = carry + one * one
        return carry

    acc[...] += lax.fori_loop(0, dst.shape[0] // 16, body, jnp.zeros((16, 128), F32))


def sum_kernel(shapes, count, head, *refs):
    g, (w0, m0, v0), refs = refs[:3], refs[3:6], refs[6:]
    out, squares, new0, refs = refs[:3], refs[3], refs[4], refs[5:]
    near, refs = refs[:3], refs[3:]
    snd, rcv, own, par, refs = refs[0:2], refs[2:4], refs[4:6], refs[6:8], refs[8:]
    first, early, refs = refs[:4], refs[4], refs[5:]
    acc, mine_sum, norms, d2d_s, d2d_r, link_s, link_r, own_sem, par_sem, out_sem, norm_s, norm_r, first_sem, early_sem, ready = refs
    layers = g[0].shape[1]
    units = [(a, l) for a in range(3) for l in range(layers)]
    end = len(units) - 1
    kind = [0, 0, 1]
    slot = {}
    for a, l in units:
        slot[a, l] = sum(1 for u in slot if kind[u[0]] == kind[a])
    me = lax.axis_index("dp")
    rep = lax.axis_index("rep")
    xn, yn, cn = place(dx=1), place(dy=1), place(dc=1)

    barrier = pltpu.get_barrier_semaphore()

    def tell(sem):
        for d in (cn, xn, yn):
            pl.semaphore_signal(sem, inc=1, device_id=(rep, d), device_id_type=MESH)

    tell(barrier)

    mine = pl.ds(pl.multiple_of(me * shapes[0][0], 16), head)
    ahead = [
        pltpu.make_async_copy(w0.at[0, mine], first[0], first_sem.at[0]),
        pltpu.make_async_copy(m0.at[0, pl.ds(0, head)], first[1], first_sem.at[1]),
        pltpu.make_async_copy(v0.at[0, pl.ds(0, head)], first[2], first_sem.at[2]),
    ]

    def split(i, j):
        n = shapes[units[i][0]][0] // 2
        if i == 0 and j < 2:
            return [(0, 16), (16, n - 16)]
        if i == end and j >= 4:
            return [(0, n - n // 5), (n - n // 5, n // 5)]
        return [(0, n)]

    def rows(u, device, h, piece):
        a, l = u
        n = shapes[a][0] // 2
        return g[a].at[0, l, pl.ds(pl.multiple_of(device * (2 * n) + h * n + piece[0], 16), piece[1])]

    def all_of(ref, sem):
        pltpu.make_async_copy(ref, ref, sem).wait()

    opening = [(0, h, p) for p in split(0, 0) for h in range(2)]
    near_sends = []
    for k, (s, h, p) in enumerate(opening):
        near_sends.append((early.at[h] if k < 2 else rows(units[0], place(*CHIPS[s], 1), h, p), par[0].at[h, pl.ds(*p)], 0, k))
    for i, (a, l) in enumerate(units):
        for s in range(4):
            if (i, s) != (0, 0):
                near_sends.append((rows(units[i], place(*CHIPS[s], 1), 0, (0, shapes[a][0])), near[a].at[l, s], a, 4 + i))
    near_sends = [
        pltpu.make_async_remote_copy(
            src_ref=src, dst_ref=dst, send_sem=d2d_s.at[a], recv_sem=d2d_r.at[k], device_id=(rep, cn), device_id_type=MESH
        )
        for src, dst, a, k in near_sends
    ]

    tasks = []
    for i in range(end + 1):
        both = [(i, s, h, p, (), j) for j, s, h in ((0, 0, 0), (1, 0, 1)) for p in split(i, j)]
        both.sort(key=lambda one: one[3][0])
        tasks += both + [(i, s, h, p, (), j) for j, s, h in ((2, 1, 0), (3, 2, 1)) for p in split(i, j)]
    for i in range(end + 1):
        for p4, p5 in zip(split(i, 4), split(i, 5)):
            tasks += [(i, 1, 1, p4, (1,), 4), (i, 2, 0, p5, (0,), 5)]
    for i in range(end + 1):
        for p4, p5 in zip(split(i, 4), split(i, 5)):
            tasks += [(i, 3, 0, p5, (2, 5), None), (i, 3, 1, p4, (3, 4), None)]

    def arrival(i, j, p):
        return link_r.at[3 * len(units) if j >= 4 and i == end and p[0] else 3 * i + j // 2]

    def link(i, j, p):
        a, l = units[i]
        k = kind[a]
        return pltpu.make_async_remote_copy(
            src_ref=snd[k].at[slot[a, l], j % 4, pl.ds(*p)],
            dst_ref=rcv[k].at[slot[a, l], j, pl.ds(*p)],
            send_sem=link_s.at[j // 4, i],
            recv_sem=arrival(i, j, p),
            device_id=(rep, xn if j % 2 == 0 else yn),
            device_id_type=MESH,
        )

    done = set()

    def once(what, wait):
        if what not in done:
            done.add(what)
            wait()

    def arrived(i, j, p):
        a, l = units[i]
        into = rcv[kind[a]].at[slot[a, l], pl.ds(j - j % 2, 2)]
        if j >= 4:
            into = into.at[:, pl.ds(*p)]
            once(("arrived", i, 4, p), lambda: all_of(into, arrival(i, j, p)))
        else:
            once(("arrived", i, j // 2), lambda: all_of(into, arrival(i, j, p)))

    def left(i):
        a, l = units[i]
        once(("left", i), lambda: all_of(snd[kind[a]].at[slot[a, l]], link_s.at[0, i]))

    loads = {}

    def load_mine(t):
        i, s, h, p, _, _ = tasks[t]
        k, b = kind[units[i][0]], t % 2
        at = pl.ds(*p) if t < 4 else pl.ds(0, p[1])
        loads[t] = [pltpu.make_async_copy(rows(units[i], place(*CHIPS[s], 0), h, p), own[k].at[b, at], own_sem.at[t if t < 4 else b])]
        loads[t][0].start()

    def load_theirs(t):
        i, s, h, p, _, _ = tasks[t]
        a, l = units[i]
        k, b = kind[a], t % 2
        all_near = near[a].at[l] if i else near[a].at[l, pl.ds(1, 3)]
        once(("near", i), lambda: all_of(all_near, d2d_r.at[4 + i]))
        at = pl.ds(h * (shapes[a][0] // 2) + p[0], p[1])
        loads[t] += [pltpu.make_async_copy(near[a].at[l, s, at], par[k].at[b, pl.ds(0, p[1])], par_sem.at[b])]
        loads[t][1].start()

    taken = [pltpu.make_async_copy(rows(units[0], place(*CHIPS[0], 1), h, (0, 16)), early.at[h], early_sem.at[0]) for h in range(2)]
    for one in taken:
        one.start()
    for t in range(4):
        load_mine(t)
    acc[...] = jnp.zeros_like(acc)
    all_of(early, early_sem.at[0])
    pl.semaphore_wait(barrier, 3)
    for one in near_sends[:4]:
        one.start()
    for t, (i, s, h, p, added, j) in enumerate(tasks):
        if t == 2:
            for one in near_sends[4:]:
                one.start()
            tell(ready.at[0])
        if t == 12:
            for one in ahead:
                one.start()
        here = t > 3 and t + 1 < len(tasks) and ("near", tasks[t + 1][0]) in done
        late = t > 2 and t + 1 < len(tasks) and not here
        if here:
            load_mine(t + 1)
            load_theirs(t + 1)
        if t in (8, 16):
            pl.semaphore_wait(ready.at[t // 8 - 1], 3)
            if t == 8:
                tell(ready.at[1])
        a, l = units[i]
        k = kind[a]
        for one in loads[t]:
            one.wait()
        if t < 4:
            near_sends[t].wait_recv()
        for r in added:
            arrived(i, r, p)
        held = pl.ds(p[0] if t < 4 else 0, p[1])
        parts = [own[k].at[t % 2, held], par[k].at[t % 2, held]]
        parts += [rcv[k].at[slot[a, l], r, pl.ds(*p)] for r in added]
        if j is None:
            dst = snd[k].at[slot[a, l], 2 + h, pl.ds(*p)]
            left(i)
            add_square(dst, parts, shapes[a][1], acc)
            store = pltpu.make_async_copy(dst, out[a].at[l, pl.ds(h * (shapes[a][0] // 2) + p[0], p[1])], out_sem.at[a])
            store.start()
        else:
            dst = snd[k].at[slot[a, l], j % 4, pl.ds(*p)]
            if j >= 4:
                left(i)
            add_into(dst, parts)
            link(i, j, p).start()
        if late:
            load_mine(t + 1)
            load_theirs(t + 1)

    ring = pl.ds(0, 7)
    mine_sum[...] = jnp.sum(acc[...], axis=0, keepdims=True)
    for k in range(1, 8):
        pltpu.make_async_remote_copy(
            src_ref=mine_sum,
            dst_ref=norms.at[me],
            send_sem=norm_s.at[0],
            recv_sem=norm_r.at[0],
            device_id=(rep, lax.rem(me + k, 8)),
            device_id_type=MESH,
        ).start()
    norms[me] = mine_sum[...]
    for one in ahead:
        one.wait()
    for a in range(3):
        all_of(out[a], out_sem.at[a])
        all_of(near[a], d2d_s.at[a])
    for i, (a, l) in enumerate(units):
        all_of(snd[kind[a]].at[slot[a, l], pl.ds(0, 2)], link_s.at[1, i])
    all_of(norms.at[ring], norm_r.at[0])
    total = norms[0]
    for d in range(1, 8):
        total = total + norms[d]
    total = jnp.sum(total, axis=1, keepdims=True)
    squares[...] = jnp.broadcast_to(total, squares.shape)

    half = snd[0].at[slot[0, 0], 2]

    for i in range(head // 16):
        r = pl.ds(i * 16, 16)
        first[3][r, :] = stepped_block(total, count, half[r, :], *(one[r, :] for one in first[:3]))[0]
        pltpu.make_async_copy(first[3].at[r], new0.at[r], first_sem.at[3]).start()
    all_of(norms.at[ring], norm_s.at[0])
    all_of(new0, first_sem.at[3])


def dma(*shape):
    return pltpu.SemaphoreType.DMA(shape)


def summed(terms, count, head, w, m, v):
    layers = terms[0].shape[1]
    shapes = [(t.shape[2] // 8, t.shape[3]) for t in terms]
    halves = [(n // 2, lanes) for n, lanes in shapes[::2]]
    counts = [2 * layers, layers]
    any_ = pl.BlockSpec(memory_space=pl.ANY)
    outs = pl.pallas_call(
        functools.partial(sum_kernel, shapes, count, head),
        out_shape=[jax.ShapeDtypeStruct((layers, *s), BF16) for s in shapes]
        + [jax.ShapeDtypeStruct((8, 128), F32)]
        + [jax.ShapeDtypeStruct((head, shapes[0][1]), BF16)]
        + [jax.ShapeDtypeStruct((layers, 4, *s), BF16) for s in shapes],
        in_specs=[any_] * 6,
        out_specs=[any_] * 3 + [pl.BlockSpec(memory_space=pltpu.VMEM)] + [any_] * 4,
        scratch_shapes=[pltpu.VMEM((n, 4, *s), BF16) for n, s in zip(counts, halves)]
        + [pltpu.VMEM((n, 6, *s), BF16) for n, s in zip(counts, halves)]
        + [pltpu.VMEM((2, *s), BF16) for s in halves] * 2
        + [pltpu.VMEM((head, shapes[0][1]), t) for t in (BF16, F32, F32, BF16)]
        + [pltpu.VMEM((2, 16, shapes[0][1]), BF16)]
        + [
            pltpu.VMEM((16, 128), F32),
            pltpu.VMEM((1, 128), F32),
            pltpu.VMEM((8, 1, 128), F32),
            dma(3),
            dma(4 + 3 * layers),
            dma(2, 3 * layers),
            dma(9 * layers + 1),
            dma(4),
            dma(2),
            dma(3),
            dma(1),
            dma(1),
            dma(4),
            dma(1),
            pltpu.SemaphoreType.REGULAR((2,)),
        ],
        compiler_params=pltpu.CompilerParams(collective_id=0, has_side_effects=True, vmem_limit_bytes=62 * 1024 * 1024),
        name="sum_terms",
    )(*terms, w, m, v)
    return outs[:3], outs[3], outs[4]


def step_kernel(count, with_weight, me, squares, g, w, m, v, *rest):
    new = stepped_block(squares[:1, :1], count, g[0], w[0], m[0], v[0])
    rest[-2][0], rest[-1][0] = new[1:]
    if with_weight:
        rest[-3][...] = new[0]


def stepped_block(squares, count, g, w, m, v):
    g = g.astype(F32) * jnp.minimum(1.0, 0.5 * lax.rsqrt(squares / count + 1e-30))
    m = 0.9 * m + 0.1 * g
    v = 0.95 * v + 0.05 * g * g
    w = w.astype(F32)
    step = m * lax.rsqrt(v + 1e-8) + 0.1 * w
    return (w - 0.02 * step).astype(BF16), m, v


def stepped(me, squares, count, unit, g, w, m, v, before, with_weight):
    layer, start, rows = unit
    whole, lanes = g.shape[1:]
    n = rows if layer and rows < whole else rows // (2 if rows == whole else 5)
    here = pl.BlockSpec((1, n, lanes), lambda i, me: (layer, start // n + i, 0))
    specs = [
        pl.BlockSpec((8, 128), lambda i, me: (0, 0)),
        here,
        pl.BlockSpec((1, n, lanes), lambda i, me: (layer, me[0] * (whole // n) + start // n + i, 0)),
        here,
        here,
    ]
    moment = jax.ShapeDtypeStruct(m.shape, F32)
    return pl.pallas_call(
        functools.partial(step_kernel, count, with_weight),
        out_shape=[jax.ShapeDtypeStruct((rows, lanes), BF16)] * with_weight + [moment, moment],
        grid_spec=pltpu.PrefetchScalarGridSpec(
            num_scalar_prefetch=1,
            grid=(rows // n,),
            in_specs=specs + [pl.BlockSpec(memory_space=pl.ANY)] * len(before),
            out_specs=[pl.BlockSpec((n, lanes), lambda i, me: (i, 0))] * with_weight + [here, here],
        ),
        input_output_aliases={6 + i: with_weight + i for i in range(len(before))},
        cost_estimate=pl.CostEstimate(flops=15 * rows * lanes, bytes_accessed=22 * rows * lanes, transcendentals=rows * lanes),
        name="adamw",
    )(me, squares, g, w, m, v, *before)


def place_kernel(places, n_before, in_vmem, *refs):
    n = len(places)
    blocks, out = refs[:n], refs[n + n_before]
    out_sem, refs = refs[n + n_before + 1], refs[n + n_before + 2 :]
    if not in_vmem:
        held, in_sem = refs
        for i in range(n):
            pltpu.make_async_copy(blocks[i], held.at[i], in_sem.at[0]).start()
        pltpu.make_async_copy(held, held, in_sem.at[0]).wait()
        blocks = [held.at[i] for i in range(n)]
    stores = []
    for i, (offset, layer, start) in enumerate(places):
        at = pl.multiple_of(place(*offset) * (out.shape[1] // 8) + start, 16)
        stores.append(pltpu.make_async_copy(blocks[i], out.at[layer, pl.ds(at, blocks[i].shape[0])], out_sem.at[i]))
        stores[-1].start()
    for one in stores:
        one.wait()


def placed(blocks, places, shape, before, in_vmem=False):
    n = len(blocks)
    any_ = pl.BlockSpec(memory_space=pl.ANY)
    scratch = [pltpu.SemaphoreType.DMA((n,))]
    if not in_vmem:
        scratch += [pltpu.VMEM((n, *blocks[0].shape), BF16), pltpu.SemaphoreType.DMA((1,))]
    return pl.pallas_call(
        functools.partial(place_kernel, places, len(before), in_vmem),
        out_shape=jax.ShapeDtypeStruct(shape, BF16),
        in_specs=[pl.BlockSpec(memory_space=pltpu.VMEM) if in_vmem else any_] * n + [any_] * len(before),
        out_specs=any_,
        scratch_shapes=scratch,
        input_output_aliases={n: 0} if before else {},
        compiler_params=pltpu.CompilerParams(vmem_limit_bytes=16 * 1024 * 1024) if in_vmem else None,
        cost_estimate=pl.CostEstimate(flops=0, bytes_accessed=4 * sum(b.size for b in blocks), transcendentals=0),
        name="place",
    )(*blocks, *before)


def send(block, dx=0, dy=0, dc=0):
    flip = 4 * dx + 2 * dy + dc
    return lax.ppermute(block, "dp", [(d, d ^ flip) for d in range(8)])


def parts_of(layers, shapes):
    units = []
    for a, (rows, _) in enumerate(shapes):
        for l in range(layers):
            cuts = 2 if (a, l) == (0, 0) else 4 if (a, l) == (2, layers - 1) else 1
            units += [(a, l, i * rows // cuts, rows // cuts) for i in range(cuts)]
    return units


def solution(mesh):
    layers, shapes = 2, [(160, 5120), (160, 5120), (640, 1280)]
    units = parts_of(layers, shapes)
    groups = []
    for i, (a, l, _, rows) in enumerate(units):
        if groups and len(groups[-1]) == 1 and units[i - 1][:2] == (a, l):
            groups[-1].append(i)
        else:
            groups.append([i])

    def step(*arrays):
        terms, weights, m, v = (arrays[i : i + 3] for i in (0, 3, 6, 9))
        count = 8 * sum(one.size for one in m)
        gradients, squares, head = summed(terms, count, units[0][3], weights[0], m[0], v[0])
        me = lax.axis_index("dp")[None]
        new_m, new_v, whole = [()] * 3, [()] * 3, [()] * 3
        first, second = [], []
        for i, (a, *unit) in enumerate(units):
            before = (new_m[a], new_v[a]) if len(new_m[a]) else ()
            *own, new_m[a], new_v[a] = stepped(me, squares, count, unit, gradients[a], weights[a], m[a], v[a], before, i > 0)
            own = own[0] if own else head
            first.append((own, send(own, dx=1), send(own, dy=1), send(own, dc=1)))
        for i, (own, x, y, c) in enumerate(first):
            far = send(y, dx=1) if i % 2 else send(x, dy=1)
            second.append((far, send(x, dc=1), send(y, dc=1)))
        for i, (a, l, start, _) in enumerate(units):
            own, x, y, c = first[i]
            far, xc, yc = second[i]
            places = [((*chip, core), l, start) for core in range(2) for chip in CHIPS[:0:-1]]
            whole[a] = placed([own, y, x, c, yc, xc], places, weights[a].shape, (whole[a],) if len(whole[a]) else ())
        for k, group in enumerate(groups):
            blocks, places = [], []
            for i in group:
                a, l, start, _ = units[i]
                far = second[i][0]
                blocks += [far, send(far, dc=1)]
                places += [((*CHIPS[0], core), l, start) for core in range(2)]
            if k + 1 == len(groups):
                whole[a] = placed(blocks[::2], places[::2], weights[a].shape, (whole[a],))
                blocks, places = blocks[1::2], places[1::2]
            whole[a] = placed(blocks, places, weights[a].shape, (whole[a],), in_vmem=True)
        return (*whole, *new_m, *new_v)

    all_of, cut = P(None, None, None), P(None, "dp", None)
    return jax.shard_map(
        step,
        mesh=mesh,
        in_specs=(P(("rep", "dp"), None, None, None),) * 3 + (all_of,) * 3 + (cut,) * 6,
        out_specs=(P("rep", None, None),) * 3 + (P("rep", "dp", None),) * 6,
        check_vma=False,
    )
```

```python
import functools

import jax
import jax.numpy as jnp
from jax import lax
from jax.experimental import pallas as pl
from jax.experimental.pallas import tpu as pltpu
from jax.sharding import PartitionSpec as P


MESH = pl.DeviceIdType.MESH
F32, BF16 = jnp.float32, jnp.bfloat16
CHIPS = ((1, 1), (1, 0), (0, 1), (0, 0))


def place(dx=0, dy=0, dc=0):
    me = lax.axis_index("dp")
    x, y, c = me // 4, lax.rem(me // 2, 2), lax.rem(me, 2)
    x = 1 - x if dx else x
    y = 1 - y if dy else y
    c = 1 - c if dc else c
    return 4 * x + 2 * y + c


def add_into(dst, parts):
    def body(i, carry):
        s = pl.ds(pl.multiple_of(i * 16, 16), 16)
        total = parts[0][s, :].astype(F32)
        for p in parts[1:]:
            total = total + p[s, :].astype(F32)
        dst[s, :] = total.astype(BF16)
        return carry

    lax.fori_loop(0, dst.shape[0] // 16, body, 0)


def add_square(dst, parts, lanes, acc):
    def body(i, carry):
        s = pl.ds(pl.multiple_of(i * 16, 16), 16)
        total = parts[0][s, :].astype(F32)
        for p in parts[1:]:
            total = total + p[s, :].astype(F32)
        total = total.astype(BF16)
        dst[s, :] = total
        total = total.astype(F32)
        for k in range(lanes // 128):
            one = total[:, k * 128 : (k + 1) * 128]
            carry = carry + one * one
        return carry

    acc[...] += lax.fori_loop(0, dst.shape[0] // 16, body, jnp.zeros((16, 128), F32))


def sum_kernel(shapes, count, head, *refs):
    g, (w0, m0, v0), refs = refs[:3], refs[3:6], refs[6:]
    out, squares, new0, refs = refs[:3], refs[3], refs[4], refs[5:]
    near, refs = refs[:3], refs[3:]
    snd, rcv, own, par, refs = refs[0:2], refs[2:4], refs[4:6], refs[6:8], refs[8:]
    first, early, refs = refs[:4], refs[4], refs[5:]
    acc, mine_sum, norms, d2d_s, d2d_r, link_s, link_r, own_sem, par_sem, out_sem, norm_s, norm_r, first_sem, early_sem, ready = refs
    layers = g[0].shape[1]
    units = [(a, l) for a in range(3) for l in range(layers)]
    end = len(units) - 1
    kind = [0, 0, 1]
    slot = {}
    for a, l in units:
        slot[a, l] = sum(1 for u in slot if kind[u[0]] == kind[a])
    me = lax.axis_index("dp")
    rep = lax.axis_index("rep")
    xn, yn, cn = place(dx=1), place(dy=1), place(dc=1)

    barrier = pltpu.get_barrier_semaphore()

    def tell(sem):
        for d in (cn, xn, yn):
            pl.semaphore_signal(sem, inc=1, device_id=(rep, d), device_id_type=MESH)

    tell(barrier)

    mine = pl.ds(pl.multiple_of(me * shapes[0][0], 16), head)
    ahead = [
        pltpu.make_async_copy(w0.at[0, mine], first[0], first_sem.at[0]),
        pltpu.make_async_copy(m0.at[0, pl.ds(0, head)], first[1], first_sem.at[1]),
        pltpu.make_async_copy(v0.at[0, pl.ds(0, head)], first[2], first_sem.at[2]),
    ]

    def split(i, j):
        n = shapes[units[i][0]][0] // 2
        if i == 0 and j < 2:
            return [(0, 16), (16, n - 16)]
        if i == end and j >= 4:
            return [(0, n - 48), (n - 48, 48)]
        return [(0, n)]

    def rows(u, device, h, piece):
        a, l = u
        n = shapes[a][0] // 2
        return g[a].at[0, l, pl.ds(pl.multiple_of(device * (2 * n) + h * n + piece[0], 16), piece[1])]

    def all_of(ref, sem):
        pltpu.make_async_copy(ref, ref, sem).wait()

    opening = [(0, h, p) for p in split(0, 0) for h in range(2)]
    near_sends = []
    for k, (s, h, p) in enumerate(opening):
        near_sends.append((early.at[h] if k < 2 else rows(units[0], place(*CHIPS[s], 1), h, p), par[0].at[h, pl.ds(*p)], 0, k))
    for i, (a, l) in enumerate(units):
        for s in range(4):
            if (i, s) != (0, 0):
                near_sends.append((rows(units[i], place(*CHIPS[s], 1), 0, (0, shapes[a][0])), near[a].at[l, s], a, 4 + i))
    near_sends = [
        pltpu.make_async_remote_copy(
            src_ref=src, dst_ref=dst, send_sem=d2d_s.at[a], recv_sem=d2d_r.at[k], device_id=(rep, cn), device_id_type=MESH
        )
        for src, dst, a, k in near_sends
    ]

    tasks = []
    for i in range(end + 1):
        both = [(i, s, h, p, (), j) for j, s, h in ((0, 0, 0), (1, 0, 1)) for p in split(i, j)]
        both.sort(key=lambda one: one[3][0])
        tasks += both + [(i, s, h, p, (), j) for j, s, h in ((2, 1, 0), (3, 2, 1)) for p in split(i, j)]
    for i in range(end + 1):
        for p4, p5 in zip(split(i, 4), split(i, 5)):
            tasks += [(i, 1, 1, p4, (1,), 4), (i, 2, 0, p5, (0,), 5)]
    for i in range(end + 1):
        for p4, p5 in zip(split(i, 4), split(i, 5)):
            tasks += [(i, 3, 0, p5, (2, 5), None), (i, 3, 1, p4, (3, 4), None)]

    def arrival(i, j, p):
        return link_r.at[3 * len(units) if j >= 4 and i == end and p[0] else 3 * i + j // 2]

    def link(i, j, p):
        a, l = units[i]
        k = kind[a]
        return pltpu.make_async_remote_copy(
            src_ref=snd[k].at[slot[a, l], j % 4, pl.ds(*p)],
            dst_ref=rcv[k].at[slot[a, l], j, pl.ds(*p)],
            send_sem=link_s.at[j // 4, i],
            recv_sem=arrival(i, j, p),
            device_id=(rep, xn if j % 2 == 0 else yn),
            device_id_type=MESH,
        )

    done = set()

    def once(what, wait):
        if what not in done:
            done.add(what)
            wait()

    def arrived(i, j, p):
        a, l = units[i]
        into = rcv[kind[a]].at[slot[a, l], pl.ds(j - j % 2, 2)]
        if j >= 4:
            into = into.at[:, pl.ds(*p)]
            once(("arrived", i, 4, p), lambda: all_of(into, arrival(i, j, p)))
        else:
            once(("arrived", i, j // 2), lambda: all_of(into, arrival(i, j, p)))

    def left(i):
        a, l = units[i]
        once(("left", i), lambda: all_of(snd[kind[a]].at[slot[a, l]], link_s.at[0, i]))

    loads = {}

    def load_mine(t):
        i, s, h, p, _, _ = tasks[t]
        k, b = kind[units[i][0]], t % 2
        at = pl.ds(*p) if t < 4 else pl.ds(0, p[1])
        loads[t] = [pltpu.make_async_copy(rows(units[i], place(*CHIPS[s], 0), h, p), own[k].at[b, at], own_sem.at[t if t < 4 else b])]
        loads[t][0].start()

    def load_theirs(t):
        i, s, h, p, _, _ = tasks[t]
        a, l = units[i]
        k, b = kind[a], t % 2
        all_near = near[a].at[l] if i else near[a].at[l, pl.ds(1, 3)]
        once(("near", i), lambda: all_of(all_near, d2d_r.at[4 + i]))
        at = pl.ds(h * (shapes[a][0] // 2) + p[0], p[1])
        loads[t] += [pltpu.make_async_copy(near[a].at[l, s, at], par[k].at[b, pl.ds(0, p[1])], par_sem.at[b])]
        loads[t][1].start()

    taken = [pltpu.make_async_copy(rows(units[0], place(*CHIPS[0], 1), h, (0, 16)), early.at[h], early_sem.at[0]) for h in range(2)]
    for one in taken:
        one.start()
    for t in range(4):
        load_mine(t)
    acc[...] = jnp.zeros_like(acc)
    all_of(early, early_sem.at[0])
    pl.semaphore_wait(barrier, 3)
    for one in near_sends[:4]:
        one.start()
    for t, (i, s, h, p, added, j) in enumerate(tasks):
        if t == 2:
            for one in near_sends[4:]:
                one.start()
            tell(ready.at[0])
        if t == 12:
            for one in ahead:
                one.start()
        here = t > 3 and t + 1 < len(tasks) and ("near", tasks[t + 1][0]) in done
        late = t > 2 and t + 1 < len(tasks) and not here
        if here:
            load_mine(t + 1)
            load_theirs(t + 1)
        if t in (8, 16):
            pl.semaphore_wait(ready.at[t // 8 - 1], 3)
            if t == 8:
                tell(ready.at[1])
        a, l = units[i]
        k = kind[a]
        for one in loads[t]:
            one.wait()
        if t < 4:
            near_sends[t].wait_recv()
        for r in added:
            arrived(i, r, p)
        held = pl.ds(p[0] if t < 4 else 0, p[1])
        parts = [own[k].at[t % 2, held], par[k].at[t % 2, held]]
        parts += [rcv[k].at[slot[a, l], r, pl.ds(*p)] for r in added]
        if j is None:
            dst = snd[k].at[slot[a, l], 2 + h, pl.ds(*p)]
            left(i)
            add_square(dst, parts, shapes[a][1], acc)
            store = pltpu.make_async_copy(dst, out[a].at[l, pl.ds(h * (shapes[a][0] // 2) + p[0], p[1])], out_sem.at[a])
            store.start()
        else:
            dst = snd[k].at[slot[a, l], j % 4, pl.ds(*p)]
            if j >= 4:
                left(i)
            add_into(dst, parts)
            link(i, j, p).start()
        if late:
            load_mine(t + 1)
            load_theirs(t + 1)

    ring = pl.ds(0, 7)
    mine_sum[...] = jnp.sum(acc[...], axis=0, keepdims=True)
    for to in [place(*chip, core) for chip in CHIPS for core in (1, 0)][:7]:
        pltpu.make_async_remote_copy(
            src_ref=mine_sum,
            dst_ref=norms.at[me],
            send_sem=norm_s.at[0],
            recv_sem=norm_r.at[0],
            device_id=(rep, to),
            device_id_type=MESH,
        ).start()
    norms[me] = mine_sum[...]
    for one in ahead:
        one.wait()
    for a in range(3):
        all_of(out[a], out_sem.at[a])
        all_of(near[a], d2d_s.at[a])
    for i, (a, l) in enumerate(units):
        all_of(snd[kind[a]].at[slot[a, l], pl.ds(0, 2)], link_s.at[1, i])
    all_of(norms.at[ring], norm_r.at[0])
    total = norms[0]
    for d in range(1, 8):
        total = total + norms[d]
    total = jnp.sum(total, axis=1, keepdims=True)
    squares[...] = jnp.broadcast_to(total, squares.shape)

    half = snd[0].at[slot[0, 0], 2]

    for i in range(head // 16):
        r = pl.ds(i * 16, 16)
        first[3][r, :] = stepped_block(total, count, half[r, :], *(one[r, :] for one in first[:3]))[0]
        pltpu.make_async_copy(first[3].at[r], new0.at[r], first_sem.at[3]).start()
    all_of(norms.at[ring], norm_s.at[0])
    all_of(new0, first_sem.at[3])


def dma(*shape):
    return pltpu.SemaphoreType.DMA(shape)


def summed(terms, count, head, w, m, v):
    layers = terms[0].shape[1]
    shapes = [(t.shape[2] // 8, t.shape[3]) for t in terms]
    halves = [(n // 2, lanes) for n, lanes in shapes[::2]]
    counts = [2 * layers, layers]
    any_ = pl.BlockSpec(memory_space=pl.ANY)
    outs = pl.pallas_call(
        functools.partial(sum_kernel, shapes, count, head),
        out_shape=[jax.ShapeDtypeStruct((layers, *s), BF16) for s in shapes]
        + [jax.ShapeDtypeStruct((8, 128), F32)]
        + [jax.ShapeDtypeStruct((head, shapes[0][1]), BF16)]
        + [jax.ShapeDtypeStruct((layers, 4, *s), BF16) for s in shapes],
        in_specs=[any_] * 6,
        out_specs=[any_] * 3 + [pl.BlockSpec(memory_space=pltpu.VMEM)] + [any_] * 4,
        scratch_shapes=[pltpu.VMEM((n, 4, *s), BF16) for n, s in zip(counts, halves)]
        + [pltpu.VMEM((n, 6, *s), BF16) for n, s in zip(counts, halves)]
        + [pltpu.VMEM((2, *s), BF16) for s in halves] * 2
        + [pltpu.VMEM((head, shapes[0][1]), t) for t in (BF16, F32, F32, BF16)]
        + [pltpu.VMEM((2, 16, shapes[0][1]), BF16)]
        + [
            pltpu.VMEM((16, 128), F32),
            pltpu.VMEM((1, 128), F32),
            pltpu.VMEM((8, 1, 128), F32),
            dma(3),
            dma(4 + 3 * layers),
            dma(2, 3 * layers),
            dma(9 * layers + 1),
            dma(4),
            dma(2),
            dma(3),
            dma(1),
            dma(1),
            dma(4),
            dma(1),
            pltpu.SemaphoreType.REGULAR((2,)),
        ],
        compiler_params=pltpu.CompilerParams(collective_id=0, has_side_effects=True, vmem_limit_bytes=62 * 1024 * 1024),
        name="sum_terms",
    )(*terms, w, m, v)
    return outs[:3], outs[3], outs[4]


def step_kernel(count, with_weight, me, squares, g, w, m, v, *rest):
    new = stepped_block(squares[:1, :1], count, g[0], w[0], m[0], v[0])
    rest[-2][0], rest[-1][0] = new[1:]
    if with_weight:
        rest[-3][...] = new[0]


def stepped_block(squares, count, g, w, m, v):
    g = g.astype(F32) * jnp.minimum(1.0, 0.5 * lax.rsqrt(squares / count + 1e-30))
    m = 0.9 * m + 0.1 * g
    v = 0.95 * v + 0.05 * g * g
    w = w.astype(F32)
    step = m * lax.rsqrt(v + 1e-8) + 0.1 * w
    return (w - 0.02 * step).astype(BF16), m, v


def stepped(me, squares, count, unit, g, w, m, v, before, with_weight):
    layer, start, rows = unit
    whole, lanes = g.shape[1:]
    n = rows if layer and rows < whole else rows // (2 if rows == whole else 5)
    here = pl.BlockSpec((1, n, lanes), lambda i, me: (layer, start // n + i, 0))
    specs = [
        pl.BlockSpec((8, 128), lambda i, me: (0, 0)),
        here,
        pl.BlockSpec((1, n, lanes), lambda i, me: (layer, me[0] * (whole // n) + start // n + i, 0)),
        here,
        here,
    ]
    moment = jax.ShapeDtypeStruct(m.shape, F32)
    return pl.pallas_call(
        functools.partial(step_kernel, count, with_weight),
        out_shape=[jax.ShapeDtypeStruct((rows, lanes), BF16)] * with_weight + [moment, moment],
        grid_spec=pltpu.PrefetchScalarGridSpec(
            num_scalar_prefetch=1,
            grid=(rows // n,),
            in_specs=specs + [pl.BlockSpec(memory_space=pl.ANY)] * len(before),
            out_specs=[pl.BlockSpec((n, lanes), lambda i, me: (i, 0))] * with_weight + [here, here],
        ),
        input_output_aliases={6 + i: with_weight + i for i in range(len(before))},
        cost_estimate=pl.CostEstimate(flops=15 * rows * lanes, bytes_accessed=22 * rows * lanes, transcendentals=rows * lanes),
        name="adamw",
    )(me, squares, g, w, m, v, *before)


def place_kernel(places, n_before, in_vmem, *refs):
    n = len(places)
    blocks, out = refs[:n], refs[n + n_before]
    out_sem, refs = refs[n + n_before + 1], refs[n + n_before + 2 :]
    if not in_vmem:
        held, in_sem = refs
        for i in range(n):
            pltpu.make_async_copy(blocks[i], held.at[i], in_sem.at[0]).start()
        pltpu.make_async_copy(held, held, in_sem.at[0]).wait()
        blocks = [held.at[i] for i in range(n)]
    stores = []
    for i, (offset, layer, start) in enumerate(places):
        at = pl.multiple_of(place(*offset) * (out.shape[1] // 8) + start, 16)
        stores.append(pltpu.make_async_copy(blocks[i], out.at[layer, pl.ds(at, blocks[i].shape[0])], out_sem.at[i]))
        stores[-1].start()
    for one in stores:
        one.wait()


def placed(blocks, places, shape, before, in_vmem=False):
    n = len(blocks)
    any_ = pl.BlockSpec(memory_space=pl.ANY)
    scratch = [pltpu.SemaphoreType.DMA((n,))]
    if not in_vmem:
        scratch += [pltpu.VMEM((n, *blocks[0].shape), BF16), pltpu.SemaphoreType.DMA((1,))]
    return pl.pallas_call(
        functools.partial(place_kernel, places, len(before), in_vmem),
        out_shape=jax.ShapeDtypeStruct(shape, BF16),
        in_specs=[pl.BlockSpec(memory_space=pltpu.VMEM) if in_vmem else any_] * n + [any_] * len(before),
        out_specs=any_,
        scratch_shapes=scratch,
        input_output_aliases={n: 0} if before else {},
        compiler_params=pltpu.CompilerParams(vmem_limit_bytes=16 * 1024 * 1024) if in_vmem else None,
        cost_estimate=pl.CostEstimate(flops=0, bytes_accessed=4 * sum(b.size for b in blocks), transcendentals=0),
        name="place",
    )(*blocks, *before)


def send(block, dx=0, dy=0, dc=0):
    flip = 4 * dx + 2 * dy + dc
    return lax.ppermute(block, "dp", [(d, d ^ flip) for d in range(8)])


def parts_of(layers, shapes):
    units = []
    for a, (rows, _) in enumerate(shapes):
        for l in range(layers):
            cuts = 2 if (a, l) == (0, 0) else 4 if (a, l) == (2, layers - 1) else 1
            units += [(a, l, i * rows // cuts, rows // cuts) for i in range(cuts)]
    return units


def solution(mesh):
    layers, shapes = 2, [(160, 5120), (160, 5120), (640, 1280)]
    units = parts_of(layers, shapes)
    groups = []
    for i, (a, l, _, rows) in enumerate(units):
        if groups and len(groups[-1]) == 1 and units[i - 1][:2] == (a, l):
            groups[-1].append(i)
        else:
            groups.append([i])

    def step(*arrays):
        terms, weights, m, v = (arrays[i : i + 3] for i in (0, 3, 6, 9))
        count = 8 * sum(one.size for one in m)
        gradients, squares, head = summed(terms, count, units[0][3], weights[0], m[0], v[0])
        me = lax.axis_index("dp")[None]
        new_m, new_v, whole = [()] * 3, [()] * 3, [()] * 3
        first, second = [], []
        for i, (a, *unit) in enumerate(units):
            before = (new_m[a], new_v[a]) if len(new_m[a]) else ()
            *own, new_m[a], new_v[a] = stepped(me, squares, count, unit, gradients[a], weights[a], m[a], v[a], before, i > 0)
            own = own[0] if own else head
            first.append((own, send(own, dx=1), send(own, dy=1), send(own, dc=1)))
        for i, (own, x, y, c) in enumerate(first):
            far = send(y, dx=1) if i % 2 else send(x, dy=1)
            second.append((far, send(x, dc=1), send(y, dc=1)))
        for i, (a, l, start, _) in enumerate(units):
            own, x, y, c = first[i]
            far, xc, yc = second[i]
            places = [((*chip, core), l, start) for core in range(2) for chip in CHIPS[:0:-1]]
            whole[a] = placed([own, y, x, c, yc, xc], places, weights[a].shape, (whole[a],) if len(whole[a]) else ())
        for k, group in enumerate(groups):
            blocks, places = [], []
            for i in group:
                a, l, start, _ = units[i]
                far = second[i][0]
                blocks += [far, send(far, dc=1)]
                places += [((*CHIPS[0], core), l, start) for core in range(2)]
            if k + 1 == len(groups):
                whole[a] = placed(blocks[::2], places[::2], weights[a].shape, (whole[a],))
                blocks, places = blocks[1::2], places[1::2]
            whole[a] = placed(blocks, places, weights[a].shape, (whole[a],), in_vmem=True)
        return (*whole, *new_m, *new_v)

    all_of, cut = P(None, None, None), P(None, "dp", None)
    return jax.shard_map(
        step,
        mesh=mesh,
        in_specs=(P(("rep", "dp"), None, None, None),) * 3 + (all_of,) * 3 + (cut,) * 6,
        out_specs=(P("rep", None, None),) * 3 + (P("rep", "dp", None),) * 6,
        check_vma=False,
    )
```
